32 devices in a mesh: dp: 4 (over y, core), fsdp: 8 (over z, x).
Axes of the slice: x: 2, y: 2, z: 4, core: 2. Of those that a mesh axis runs over, the one named last changes fastest.
Arguments:
- states: bfloat16 [32, 1024, 512], P(('dp', 'fsdp')), may hold values from -6 to 6
- params: float32 [3150848], P(('dp', 'fsdp')), may hold values from -2 to 2
- first_moment: float32 [3150848], P(('dp', 'fsdp')), may hold values from -2 to 2
- second_moment: float32 [3150848], P(('dp', 'fsdp')), may hold values from 0.001 to 0.064
- ema_params: float32 [3150848], P(('dp', 'fsdp')), may hold values from -2 to 2
- lengths: int32 [32], P(('dp', 'fsdp')), may hold values from 64 to 1024, as said below
- halt_counts: int32 [32, 1024], P(('dp', 'fsdp')), may hold values from 1 to 2
- cotangent: bfloat16 [32, 1024, 512], P(('dp', 'fsdp')), may hold values from -6 to 6
Outputs:
- final_states: float32 [32, 1024, 512], P(('dp', 'fsdp'))
- input_grad: float32 [32, 1024, 512], P(('dp', 'fsdp'))
- param_grad: float32 [3150848], P(('dp', 'fsdp'))
- grad_norm: float32 [1], replicated
- new_params: float32 [3150848], P(('dp', 'fsdp'))
- new_first: float32 [3150848], P(('dp', 'fsdp'))
- new_second: float32 [3150848], P(('dp', 'fsdp'))
- new_ema: float32 [3150848], P(('dp', 'fsdp'))
- params_low: bfloat16 [3150848], P(('dp', 'fsdp'))
The draws below stay inside these ranges and needn't reach their ends.
Inputs may be any that keep to these rules, and one draw needn't show every extreme that they name: `lengths`: some row is exactly 1024 long and another exactly 64.
All inputs are finite; a program needn't handle non-finite values.
Results may differ from the reference program's by a relative error of at most 0.011.
Values may be sent and summed in bfloat16 or wider, within the bound.
No kernel may reach another device: no remote copies, remote signals or barrier semaphores. Data moves between devices by JAX's collectives and lax.ppermute only.
A program may use at most 384 MiB of HBM per device.

```python
import jax
import jax.numpy as jnp
from jax import lax

D = 512
FF = 2048
HEADS = 8
SEQ = 1024
LEN_MIN = 64
PONDER = 2
ADAM_STEP = 4
BATCH = 32
QKV_END = 786432
OUT_END = 1048576
UP_END = 2097152
DOWN_END = 3145728
NPARAM = 3150848


def layout_scales():
    index_all = jnp.arange(NPARAM, dtype=jnp.int32)
    vector_row = (index_all - DOWN_END) // D
    is_vector = index_all >= DOWN_END
    is_gain = is_vector & ((vector_row == 0) | (vector_row == 2))
    scale_all = jnp.where(index_all < QKV_END, D ** (-0.5), jnp.where(index_all < OUT_END, 4.0 * D ** (-0.5), jnp.where(index_all < UP_END, D ** (-0.5), FF ** (-0.5))))
    scale_all = jnp.where(is_vector, jnp.where(is_gain, 0.1, jnp.where(vector_row == 5, 0.5 * D ** (-0.5), 0.2)), scale_all)
    offset_all = jnp.where(is_gain, 1.0, 0.0)
    grad_unit = jnp.where(is_vector, 4.0, 1.0)
    return (scale_all.astype(jnp.float32), offset_all.astype(jnp.float32), grad_unit.astype(jnp.float32))


def normal_noise(noise_key):
    return jnp.clip(jax.random.normal(noise_key, (NPARAM,), jnp.float32), -4.0, 4.0)


def draw_params(key, part):
    scale_all, offset_all, grad_unit = layout_scales()
    noise_key = jax.random.fold_in(key, 11)
    noise_all = normal_noise(noise_key)
    return offset_all + scale_all * noise_all


def draw_ema_params(key, part):
    scale_all, offset_all, grad_unit = layout_scales()
    noise_key = jax.random.fold_in(key, 12)
    noise_all = normal_noise(noise_key)
    return offset_all + scale_all * noise_all


def draw_first_moment(key, part):
    scale_all, offset_all, grad_unit = layout_scales()
    noise_key = jax.random.fold_in(key, 13)
    noise_all = normal_noise(noise_key)
    return 0.11 * grad_unit * noise_all


def draw_second_moment(key, part):
    scale_all, offset_all, grad_unit = layout_scales()
    noise_key = jax.random.fold_in(key, 14)
    factor_all = jnp.exp(jax.random.uniform(noise_key, (NPARAM,), jnp.float32, -0.6931472, 0.6931472))
    return 0.002 * grad_unit * grad_unit * factor_all


def draw_lengths(key, part):
    length_key = jax.random.fold_in(key, 15)
    first_key, second_key = jax.random.split(length_key)
    drawn = jax.random.randint(first_key, (BATCH,), LEN_MIN, SEQ + 1, dtype=jnp.int32)
    chosen = jax.random.randint(second_key, (), 0, BATCH, dtype=jnp.int32)
    row_index = jnp.arange(BATCH, dtype=jnp.int32)
    drawn = jnp.where(row_index == chosen, SEQ, drawn)
    return jnp.where(row_index == (chosen + 1) % BATCH, LEN_MIN, drawn)


def touch_ends(array, own_key, least, high):
    place = [jax.random.randint(jax.random.fold_in(own_key, axis), (), 0, length) for axis, length in enumerate(array.shape)]
    widest = array.shape.index(max(array.shape))
    neighbour = place[:widest] + [(place[widest] + 1) % array.shape[widest]] + place[widest + 1:]
    return array.at[tuple(place)].set(least).at[tuple(neighbour)].set(high)


def level_of(own_key, extent, cuts, least, largest):
    level, own = 1.0, jax.random.fold_in(own_key, 6)
    for position, parts in cuts:
        draws = jnp.exp(jax.random.uniform(jax.random.fold_in(own, position), (parts,), jnp.float32, least / len(cuts), largest / len(cuts)))
        level = level * jnp.repeat(draws, extent[position] // parts).reshape([-1 if axis == position else 1 for axis in range(len(extent))])
    return level


def noise(stream_key, dims, deviation, bound, shards=(), held_as=jnp.bfloat16):
    level = level_of(stream_key, dims, shards, -0.22, 0.18) if shards else 1.0
    values = jax.random.normal(stream_key, dims, jnp.float32) * deviation * level
    return jnp.minimum(jnp.maximum(values, -bound), bound).astype(held_as)


def setup_inputs(seed: int = 0) -> dict:
    splits = jax.random.split(jax.random.key(seed), 9)
    states = noise(splits[0], (BATCH, SEQ, D), 1.0, 6.0, ((0, 32),))
    params = draw_params(jax.random.fold_in(splits[8], 71), 0)
    first_moment = draw_first_moment(jax.random.fold_in(splits[8], 71), 0)
    second_moment = draw_second_moment(jax.random.fold_in(splits[8], 71), 0)
    ema_params = draw_ema_params(jax.random.fold_in(splits[8], 71), 0)
    lengths = draw_lengths(jax.random.fold_in(splits[8], 71), 0)
    halt_counts = touch_ends(jax.random.randint(splits[6], (BATCH, SEQ), 1, PONDER + 1), jax.random.fold_in(splits[6], 1), 1, PONDER).astype(jnp.int32)
    cotangent = noise(splits[7], (BATCH, SEQ, D), 1.0, 6.0, ((0, 32),))
    return dict(states=states, params=params, first_moment=first_moment, second_moment=second_moment, ema_params=ema_params, lengths=lengths, halt_counts=halt_counts, cotangent=cotangent)


@jax.custom_vjp
def low(v):
    return lax.optimization_barrier(v.astype(jnp.bfloat16)).astype(jnp.float32)

@jax.custom_vjp
def low_back(v):
    return v

def low_keep(v):
    return (low(v), None)

def low_pass(kept, grad):
    return (grad,)

def back_keep(v):
    return (v, None)

def back_low(kept, grad):
    return (low(grad),)
low.defvjp(low_keep, low_pass)
low_back.defvjp(back_keep, back_low)
NORM_EPSILON = 1e-05
HALT_SHIFT = -1.0
BETA_FIRST = 0.9
BETA_SECOND = 0.999
ADAM_EPSILON = 1e-08
EMA_DECAY = 0.999
WEIGHT_DECAY = 0.1
RATE_MATRIX = 0.1
RATE_VECTOR = 1.0
MASK_FILL = -1000000000.0
HIGHEST = lax.Precision.HIGHEST

def layer_norm(inputs, gain, shift):
    centred = inputs - lax.optimization_barrier(jnp.mean(inputs, axis=-1, keepdims=True))
    normed_hat = centred * lax.rsqrt(lax.optimization_barrier(jnp.mean(centred * centred, axis=-1, keepdims=True)) + NORM_EPSILON)
    return normed_hat * gain + shift

def unpack(flat):
    w_qkv = flat[:QKV_END].reshape(D, 3 * D)
    w_out = flat[QKV_END:OUT_END].reshape(D, D)
    w_up = flat[OUT_END:UP_END].reshape(D, FF)
    w_down = flat[UP_END:DOWN_END].reshape(FF, D)
    vectors = flat[DOWN_END:].reshape(6 + FF // D, D)
    return (w_qkv, w_out, w_up, w_down, vectors)

def shared_block(current, weights, key_valid):
    w_qkv, w_out, w_up, w_down, vectors = weights
    head_size = D // HEADS
    normed = low(layer_norm(current, vectors[0], vectors[1]))
    projected = low(low_back(jnp.dot(normed, w_qkv, precision=HIGHEST)))
    head_parts = projected.reshape(SEQ, 3, HEADS, head_size)
    scores = jnp.einsum('qhd,khd->hqk', head_parts[:, 0], head_parts[:, 1], precision=HIGHEST) * head_size ** (-0.5)
    scores = jnp.where(key_valid[None, None, :], low_back(scores), MASK_FILL)
    attention = low(jax.nn.softmax(scores, axis=-1))
    mixed = jnp.einsum('hqk,khd->qhd', attention, head_parts[:, 2], precision=HIGHEST).reshape(SEQ, D)
    mixed = low(low_back(mixed))
    middle = current + low_back(jnp.dot(mixed, w_out, precision=HIGHEST))
    normed_two = low(layer_norm(middle, vectors[2], vectors[3]))
    hidden_pre = low_back(jnp.dot(normed_two, w_up, precision=HIGHEST) + vectors[6:].reshape(FF))
    hidden = low(jax.nn.gelu(hidden_pre, approximate=False))
    return middle + low_back(jnp.dot(hidden, w_down, precision=HIGHEST) + vectors[4])

def row_loss(state_first, flat, length, counts, cotangent_row):
    weights = unpack(low(flat))
    halt_weight = weights[4][5]
    key_valid = jnp.arange(SEQ) < length
    valid_float = key_valid.astype(jnp.float32)
    current = state_first
    step_states = []
    kept_halts = []
    for ponder_step in range(PONDER):
        updated = shared_block(current, weights, key_valid)
        current = jnp.where((counts > ponder_step)[:, None], updated, current)
        halting = jax.nn.sigmoid(jnp.dot(current, halt_weight, precision=HIGHEST) + HALT_SHIFT)
        step_states.append(current)
        kept_halts.append(jnp.where(counts > ponder_step + 1, halting, 0.0))
    remainder = 1.0 - sum(kept_halts)
    final = jnp.zeros_like(state_first)
    for ponder_step in range(PONDER):
        share = kept_halts[ponder_step] + jnp.where(counts == ponder_step + 1, remainder, 0.0)
        final = final + share[:, None] * step_states[ponder_step]
    final = final * valid_float[:, None]
    loss_value = jnp.sum(cotangent_row * final)
    return (loss_value, final)

def reference(states, params, first_moment, second_moment, ema_params, lengths, halt_counts, cotangent):
    group_rows = 4

    def group_loss(state_group, flat, length_group, count_group, cotangent_group):
        losses, finals = jax.vmap(row_loss, in_axes=(0, None, 0, 0, 0))(state_group, flat, length_group, count_group, cotangent_group)
        return (jnp.sum(losses), finals)

    def scan_step(grad_total, pieces):
        state_group, length_group, count_group, cotangent_group = pieces

        def closed(inputs, flat):
            return group_loss(inputs, flat, length_group, count_group, cotangent_group)
        loss_value, pullback, finals = jax.vjp(closed, state_group, params, has_aux=True)
        input_grad, flat_grad = pullback(jnp.ones_like(loss_value))
        return (grad_total + flat_grad, (finals, input_grad))
    shaped = (states.astype(jnp.float32).reshape(BATCH // group_rows, group_rows, SEQ, D), lengths.reshape(BATCH // group_rows, group_rows), halt_counts.reshape(BATCH // group_rows, group_rows, SEQ), cotangent.astype(jnp.float32).reshape(BATCH // group_rows, group_rows, SEQ, D))
    raw_grad, (finals, input_grads) = lax.scan(scan_step, jnp.zeros((NPARAM,), jnp.float32), shaped)
    grad_norm = jnp.sqrt(jnp.sum(raw_grad * raw_grad))
    clip_bound = NPARAM ** 0.5
    clipped = raw_grad * (clip_bound / jnp.maximum(grad_norm, clip_bound))
    new_first = BETA_FIRST * first_moment + (1.0 - BETA_FIRST) * clipped
    new_second = BETA_SECOND * second_moment + (1.0 - BETA_SECOND) * clipped * clipped
    first_hat = new_first / (1.0 - BETA_FIRST ** ADAM_STEP)
    second_hat = new_second / (1.0 - BETA_SECOND ** ADAM_STEP)
    matrix = jnp.arange(NPARAM) < DOWN_END
    step_rate = jnp.where(matrix, RATE_MATRIX, RATE_VECTOR)
    decay_rate = jnp.where(matrix, WEIGHT_DECAY, 0.0)
    new_params = params - step_rate * (first_hat / (jnp.sqrt(second_hat) + ADAM_EPSILON) + decay_rate * params)
    average_decay = min(EMA_DECAY, (1.0 + ADAM_STEP) / (10.0 + ADAM_STEP))
    new_ema = average_decay * ema_params + (1.0 - average_decay) * new_params
    return (finals.reshape(BATCH, SEQ, D), input_grads.reshape(BATCH, SEQ, D), clipped, grad_norm.reshape(1), new_params, new_first, new_second, new_ema, new_params.astype(jnp.bfloat16))
```

```python
import functools
import math

import jax
import jax.numpy as jnp
import numpy as np
from jax import lax
from jax.experimental import pallas as pl
from jax.experimental.pallas import tpu as pltpu
from jax.sharding import PartitionSpec as P

D = 512
FF = 2048
HEADS = 8
SEQ = 1024
ADAM_STEP = 4
QKV_END = 786432
OUT_END = 1048576
UP_END = 2097152
DOWN_END = 3145728
NPARAM = 3150848

NORM_EPSILON = 1e-05
HALT_SHIFT = -1.0
BETA_FIRST = 0.9
BETA_SECOND = 0.999
ADAM_EPSILON = 1e-08
EMA_DECAY = 0.999
WEIGHT_DECAY = 0.1
RATE_MATRIX = 0.1
RATE_VECTOR = 1.0

BLOCK = 256
BLOCKS = SEQ // BLOCK
UNIT = 128
SIZES_LENGTH = (512,)
SIZES_ATTEND = (256, 128)
SIZES_SHIFTED = (128,)
SIZES_ATTEND_BACK = (256, 128)
SIZES_FEED = (512, 128)
SIZES_BACK = (512, 128)
PAIRS = HEADS // 2
PAIR = 128
SCORE_SCALE = 0.125
SCORE_LOG2 = SCORE_SCALE * math.log2(math.e)

f32 = jnp.float32
bf16 = jnp.bfloat16
i32 = jnp.int32

CHUNK = 192
DEVICES = 32
ROWS_A = 64
ROWS_B = 144
EXTRA = 16
PACKED = CHUNK + EXTRA
PLANE = [(0, 0), (1, 0), (0, 1), (1, 1)]
UP_SEGMENTS = [(0, 16, 0)] + [(64 + CHUNK * n, 48, 16 + 48 * n) for n in range(10)] + [(64 + CHUNK * 10, 16, 496)]


def dot(left, right):
    return jnp.dot(left, right, preferred_element_type=f32)


def dot_nt(left, right):
    return lax.dot_general(left, right, (((1,), (1,)), ((), ())), preferred_element_type=f32)


def dot_tn(left, right):
    return lax.dot_general(left, right, (((0,), (0,)), ((), ())), preferred_element_type=f32)


def iota(shape, axis):
    return lax.broadcasted_iota(i32, shape, axis)


def normalize(inputs):
    centred = inputs - jnp.mean(inputs, axis=-1, keepdims=True)
    rho = lax.rsqrt(jnp.mean(centred * centred, axis=-1, keepdims=True) + NORM_EPSILON)
    return centred * rho, rho


def norm_backward(grad_out, hat, rho, gain):
    grad_hat = grad_out * gain
    return rho * (
        grad_hat
        - jnp.mean(grad_hat, axis=-1, keepdims=True)
        - hat * jnp.mean(grad_hat * hat, axis=-1, keepdims=True)
    )


def gelu_parts(pre):
    cumulative = 0.5 + 0.5 * lax.erf(pre * 0.7071067811865476)
    density = jnp.exp2(pre * pre * (-0.5 * math.log2(math.e))) * 0.3989422804014327
    return pre * cumulative, cumulative + pre * density


def qkv_weight(ref, j):
    return jnp.concatenate([ref[CHUNK * n + 64 * j : CHUNK * n + 64 * (j + 1), :] for n in range(8)], axis=0)


def up_weight(ref, j):
    return jnp.concatenate(
        [ref[2048 + at + rows * j : 2048 + at + rows * (j + 1), :] for at, rows, _ in UP_SEGMENTS], axis=0
    )


def prepare_kernel(
    length_ref, index_ref, count_ref, state_ref, cotangent_ref, place_ref, states_out, cotangent_out, meta_ref
):
    length = length_ref[0]
    token = iota((1, SEQ), 1)
    valid = token < length
    two = jnp.where(valid & (count_ref[...] >= 2), 1.0, 0.0)
    one = jnp.where(valid & (count_ref[...] < 2), 1.0, 0.0)
    masks = jnp.concatenate([two, one, jnp.zeros((6, SEQ), f32)], axis=0).astype(bf16)
    earlier = jnp.where(iota((SEQ, SEQ), 0) < iota((SEQ, SEQ), 1), 1.0, 0.0).astype(bf16)
    ranks = dot(masks, earlier)
    n_two = jnp.sum(two)
    place = jnp.where(
        two > 0.0, ranks[0:1, :], jnp.where(one > 0.0, n_two + ranks[1:2, :], token.astype(f32))
    )
    place_ref[...] = jnp.broadcast_to(place, (8, SEQ))
    meta_ref[0] = n_two.astype(i32)
    meta_ref[1] = length
    for n in range(4):
        meta_ref[2 + n] = index_ref[n]

    def sort(block, carried):
        rows = pl.ds(pl.multiple_of(block * BLOCK, BLOCK), BLOCK)
        pick = jnp.where((iota((BLOCK, SEQ), 0) + block * BLOCK).astype(f32) == place, 1.0, 0.0).astype(bf16)
        states_out[rows, :] = dot(pick, state_ref[...]).astype(bf16)
        cotangent_out[rows, :] = dot(pick, cotangent_ref[...]).astype(bf16)
        return carried

    lax.fori_loop(0, BLOCKS, sort, 0)


def prepare(lengths, place_index, counts, states, cotangent):
    return pl.pallas_call(
        prepare_kernel,
        out_shape=(
            jax.ShapeDtypeStruct((8, SEQ), f32),
            jax.ShapeDtypeStruct((SEQ, D), bf16),
            jax.ShapeDtypeStruct((SEQ, D), bf16),
            jax.ShapeDtypeStruct((6,), i32),
        ),
        in_specs=[
            pl.BlockSpec(memory_space=pltpu.SMEM),
            pl.BlockSpec(memory_space=pltpu.SMEM),
            pl.BlockSpec(memory_space=pltpu.VMEM),
            pl.BlockSpec(memory_space=pltpu.VMEM),
            pl.BlockSpec(memory_space=pltpu.VMEM),
        ],
        out_specs=(
            pl.BlockSpec(memory_space=pltpu.VMEM),
            pl.BlockSpec(memory_space=pltpu.VMEM),
            pl.BlockSpec(memory_space=pltpu.VMEM),
            pl.BlockSpec(memory_space=pltpu.SMEM),
        ),
        cost_estimate=pl.CostEstimate(flops=6 * 10**9, transcendentals=0, bytes_accessed=4 * 10**6),
        name="prepare",
    )(lengths, place_index, counts, states, cotangent)


def restore_kernel(place_ref, sorted_ref, out_ref, columns, high, lower):
    columns[...] = jnp.broadcast_to(place_ref[0:1, :], (PAIR, SEQ)).T
    high[...] = sorted_ref[...].astype(bf16)
    lower[...] = (sorted_ref[...] - high[...].astype(f32)).astype(bf16)

    def unsort(block, carried):
        rows = pl.ds(pl.multiple_of(block * BLOCK, BLOCK), BLOCK)
        pick = jnp.concatenate(
            [
                jnp.where(columns[rows, :] == (iota((BLOCK, PAIR), 1) + PAIR * n).astype(f32), 1.0, 0.0).astype(bf16)
                for n in range(SEQ // PAIR)
            ],
            axis=1,
        )
        out_ref[rows, :] = dot(pick, high[...]) + dot(pick, lower[...])
        return carried

    lax.fori_loop(0, BLOCKS, unsort, 0)


def restore(place, array, name):
    return pl.pallas_call(
        restore_kernel,
        out_shape=jax.ShapeDtypeStruct((SEQ, D), f32),
        in_specs=[pl.BlockSpec(memory_space=pltpu.VMEM)] * 2,
        out_specs=pl.BlockSpec(memory_space=pltpu.VMEM),
        scratch_shapes=[pltpu.VMEM((SEQ, PAIR), f32), pltpu.VMEM((SEQ, D), bf16), pltpu.VMEM((SEQ, D), bf16)],
        cost_estimate=pl.CostEstimate(flops=6 * 10**9, transcendentals=0, bytes_accessed=4 * 10**6),
        name=name,
    )(place, array)


def next_rows(chunk, qkv_sum, out_sum, up_sum, packed, vector_sum):
    after = chunk + 1
    if after == DEVICES:
        return vector_sum[...]
    if after < 8:
        blocks = [qkv_sum[j, 64 * after : 64 * after + 8, :] for j in range(3)]
    elif after < 11:
        at = CHUNK * after - 1536
        return out_sum[at : at + 16, :]
    elif after < 22:
        first = 16 + 48 * (after - 11)
        blocks = [up_sum[j, first : first + 8, :] for j in range(4)]
    else:
        return packed[PACKED * after : PACKED * after + 16, :].astype(f32)
    width = len(blocks)
    rows = [blocks[r % width][r // width : r // width + 1, :] for r in range(10)]
    return jnp.concatenate(rows + [jnp.zeros((6, D), f32)], axis=0)


def chunk_of(meta, dy, dc, dz, dx):
    return (((meta[2] ^ dy) * 2 + (meta[3] ^ dc)) * 4 + (meta[4] ^ dz)) * 2 + (meta[5] ^ dx)


def shape_of(*shape, dtype=f32):
    return jax.ShapeDtypeStruct(shape, dtype)


def column_sum(array):
    return jnp.sum(array, axis=0, keepdims=True)


def layer_kernel(meta, states_ref, cotangent_ref, *refs):
    pieces = refs[:16]
    (
        final_out, carry, keep_a, send_a, keep_b, send_b, spill,
        matrices, extras, vectors,
        state, projected, mixed, middle, hidden, mixed_grad, projected_grad, logs, centres,
        qkv_sum, out_sum, up_sum, down_sum, vector_sum, first_key, norm_peak, key_sum, value_sum, turned, in_sem, spill_sem, out_sem,
    ) = refs[16:]
    n_two, length = meta[0], meta[1]
    lower = iota((1, PAIR), 1) < 64
    own = [lower, ~lower]

    def at_rows(start, size):
        return pl.ds(pl.multiple_of(start, UNIT), size)

    def hidden_rows(j, start, size):
        return pl.ds(pl.multiple_of(j * SEQ + start, UNIT), size)

    def over_rows(rows, sizes, body):
        def loop(first, size, count):
            def step(n, carried):
                body(first + n * size, size)
                return carried

            lax.fori_loop(0, count, step, 0)
            return first + count * size

        large = sizes[0]
        if len(sizes) == 1:
            return loop(0, large, (rows + large - 1) // large)
        covered = loop(0, large, (rows + large // 2 - 1) // large)
        return loop(covered, sizes[1], (jnp.maximum(rows - covered, 0) + sizes[1] - 1) // sizes[1])

    def rest_rows(covered, body):
        def step(n, carried):
            body(n * UNIT, UNIT)
            return carried

        lax.fori_loop(covered // UNIT, SEQ // UNIT, step, 0)

    def weight_qkv(j):
        return qkv_weight(matrices, j)

    def weight_out():
        return matrices[1536:2048, :]

    def weight_up(j):
        return up_weight(matrices, j)

    def weight_down(j):
        return matrices[4096 + D * j : 4096 + D * (j + 1), :]

    def vector(index):
        return vectors[index : index + 1, :]

    def add_vector(index, value):
        vector_sum[index : index + 1, :] += value

    def query_rows(step):
        return jnp.where(step == 0, length, n_two)

    def row_index(start, size):
        return iota((size, 1), 0) + start

    arriving = []
    for dc in range(2):
        for plane, (dy, dx) in enumerate(PLANE):
            for dz in range(4):
                chunk = chunk_of(meta, dy, dc, dz, dx)
                row = pl.multiple_of(chunk * CHUNK, CHUNK)
                part_a, part_b = pieces[4 * dc + dz].at[plane], pieces[8 + 4 * dc + plane].at[dz]
                for source, target in (
                    (part_a, matrices.at[pl.ds(row, ROWS_A), :]),
                    (part_b.at[: CHUNK - ROWS_A, :], matrices.at[pl.ds(row + ROWS_A, CHUNK - ROWS_A), :]),
                    (part_b.at[CHUNK - ROWS_A :, :], extras.at[chunk]),
                ):
                    copy = pltpu.make_async_copy(source, target, in_sem.at[len(arriving)])
                    copy.start()
                    arriving.append(copy)

    for total in (qkv_sum, out_sum, up_sum, down_sum, vector_sum):
        total[...] = jnp.zeros_like(total)

    mixed[...] = jnp.zeros_like(mixed)
    state[0] = states_ref[...].astype(f32)
    state[1] = jnp.zeros((SEQ, D), f32)
    for copy in arriving:
        copy.wait()

    def complete(row, value):
        rows = value.shape[0]
        matrices[row : row + rows, :] = (matrices[row : row + rows, :].astype(f32) + value).astype(bf16)

    for n in range(1, DEVICES):
        value = extras[n - 1].astype(f32)
        if n < 8 or 11 <= n < 22:
            width, stride = (3, 64) if n < 8 else (4, 48 if n < 21 else 16)
            for j in range(width):
                rows = jnp.concatenate([value[4 * j : 4 * j + 4, :], jnp.zeros((4, D), f32)], axis=0)
                complete(CHUNK * n + stride * j, rows)
        else:
            complete(CHUNK * n, value)
    vectors[...] = extras[DEVICES - 1].astype(f32)

    heads = jnp.where(iota((D, PAIR), 0) // 64 == iota((D, PAIR), 1), 1.0, 0.0).astype(bf16)

    def project(step):
        def body(start, size):
            rows = at_rows(start, size)
            hat, _ = normalize(state[step, rows, :])
            normed_low = (hat * vector(0) + vector(1)).astype(bf16)
            queries = dot(normed_low, weight_qkv(0))
            projected[step, rows, 0:D] = queries.astype(bf16)
            keys = dot(normed_low, weight_qkv(1))
            for index, array in enumerate((queries, keys)):
                norms = dot((array * array).astype(bf16), heads)
                norm_peak[index : index + 1, :] = jnp.maximum(
                    norm_peak[index : index + 1, :], jnp.max(norms, axis=0, keepdims=True)
                )

            @pl.when(start == 0)
            def _():
                first_key[...] = jnp.broadcast_to(keys[0:1, :], first_key.shape)

            inside = row_index(start, size) < length
            projected[step, rows, D : 2 * D] = jnp.where(inside, keys, first_key[0:1, :]).astype(bf16)
            values = dot(normed_low, weight_qkv(2))
            projected[step, rows, 2 * D : 3 * D] = jnp.where(inside, values, 0.0).astype(bf16)

        def fill(start, size):
            rows = at_rows(start, size)
            projected[step, rows, D : 2 * D] = jnp.broadcast_to(first_key[0:1, :], (size, D)).astype(bf16)
            projected[step, rows, 2 * D : 3 * D] = jnp.zeros((size, D), bf16)

        norm_peak[...] = jnp.zeros_like(norm_peak)
        rest_rows(over_rows(length, SIZES_LENGTH, body), fill)

    def attend_pair(step, start, size, pair, shifted):
        rows = at_rows(start, size)
        ones = jnp.where(iota((SEQ, 1), 0) < length, 1.0, 0.0).astype(bf16)
        queries = projected[step, rows, pl.ds(pair * PAIR, PAIR)]
        keys = projected[step, :, pl.ds(D + pair * PAIR, PAIR)]
        values = projected[step, :, pl.ds(2 * D + pair * PAIR, PAIR)]
        peaks, sums = [], []
        for half in range(2):
            scores = dot_nt(jnp.where(own[half], queries, jnp.zeros_like(queries)), keys) * SCORE_LOG2
            if shifted:
                peaks.append(jnp.max(scores, axis=-1, keepdims=True))
                scores = scores - peaks[half]
            sums.append(dot(jnp.exp2(scores).astype(bf16), jnp.where(own[half], values, ones)))
        total = jnp.where(lower, pltpu.roll(sums[0], 64, 1), pltpu.roll(sums[1], 64, 1))
        mixed[step, rows, pl.ds(pair * PAIR, PAIR)] = (jnp.where(lower, sums[0], sums[1]) / total).astype(bf16)
        log = jnp.log2(total)
        if shifted:
            log = log + jnp.where(lower, peaks[0], peaks[1])
        log = log.T
        for unit in range(size // UNIT):
            columns = slice(unit * UNIT, (unit + 1) * UNIT)
            logs[step, start // UNIT + unit, pl.ds(2 * pair, 1), :] = log[0:1, columns]
            logs[step, start // UNIT + unit, pl.ds(2 * pair + 1, 1), :] = log[64:65, columns]

    def attend(step):
        bound = jnp.max(norm_peak[0:1, :] * norm_peak[1:2, :])
        plain = bound * (1.02 * SCORE_LOG2) ** 2 < 60.0**2

        @pl.when(plain)
        def _():
            def body(start, size):
                for pair in range(PAIRS):
                    attend_pair(step, start, size, pair, False)

            over_rows(query_rows(step), SIZES_ATTEND, body)

        @pl.when(~plain)
        def _():
            def body(start, size):
                def each(pair, carried):
                    attend_pair(step, start, size, pl.multiple_of(pair, 1), True)
                    return carried

                lax.fori_loop(0, PAIRS, each, 0)

            over_rows(query_rows(step), SIZES_SHIFTED, body)

    def feed_forward(step):
        def body(start, size):
            rows = at_rows(start, size)
            between = state[step, rows, :] + dot(mixed[step, rows, :], weight_out())
            middle[step, rows, :] = between
            hat, _ = normalize(between)
            normed_low = (hat * vector(2) + vector(3)).astype(bf16)
            output = between + vector(4)
            for j in range(4):
                value, slope = gelu_parts(dot(normed_low, weight_up(j)) + vector(6 + j))
                value_low = value.astype(bf16)
                hidden[hidden_rows(j, start, size), :] = value_low
                hidden[hidden_rows(4 + j, start, size), :] = slope.astype(bf16)
                output = output + dot(value_low, weight_down(j))
            state[step + 1, rows, :] = output

        over_rows(query_rows(step), SIZES_FEED, body)

    def save():
        return pltpu.make_async_copy(hidden, spill, spill_sem)

    def fetch():
        return pltpu.make_async_copy(spill, hidden, spill_sem)

    def forward(step, carried):
        project(step)
        attend(step)

        @pl.when(step == 1)
        def _():
            save().wait()

        feed_forward(step)

        @pl.when(step == 0)
        def _():
            save().start()

        return carried

    lax.fori_loop(0, 2, forward, 0)

    def mix(start, size):
        rows = at_rows(start, size)
        row = row_index(start, size)
        two, valid = row < n_two, row < length
        before = state[1, rows, :]
        after = jnp.where(two, state[2, rows, :], before)
        halting = jax.nn.sigmoid(jnp.sum(before * vector(5), axis=-1, keepdims=True) + HALT_SHIFT)
        share_one = jnp.where(two, halting, 1.0)
        share_two = jnp.where(two, 1.0 - halting, 0.0)
        final_out[rows, :] = jnp.where(valid, share_one * before + share_two * after, 0.0)
        grad_final = jnp.where(valid, cotangent_ref[rows, :].astype(f32), 0.0)
        first_sum = jnp.sum(grad_final * before, axis=-1, keepdims=True)
        second_sum = jnp.sum(grad_final * after, axis=-1, keepdims=True)
        logit_grad = jnp.where(two, (first_sum - second_sum) * halting * (1.0 - halting), 0.0)
        add_vector(5, column_sum(jnp.where(valid, logit_grad * before, 0.0)))
        carry[rows, :] = share_two * grad_final
        state[2, rows, :] = jnp.where(valid, share_one * grad_final + logit_grad * vector(5), 0.0)

    def blank(start, size):
        rows = at_rows(start, size)
        final_out[rows, :] = jnp.zeros((size, D), f32)
        carry[rows, :] = jnp.zeros((size, D), f32)

    rest_rows(over_rows(length, SIZES_LENGTH, mix), blank)

    def feed_back(step):
        def body(start, size):
            rows = at_rows(start, size)
            grad = carry[rows, :]
            branch = grad.astype(bf16)
            add_vector(4, column_sum(branch.astype(f32)))
            hat, rho = normalize(middle[step, rows, :])
            normed_low = (hat * vector(2) + vector(3)).astype(bf16)
            normed_grad = jnp.zeros((size, D), f32)
            for j in range(4):
                down_sum[j] += dot_tn(branch, hidden[hidden_rows(j, start, size), :])
                slope = hidden[hidden_rows(4 + j, start, size), :].astype(f32)
                pre_grad = (dot_nt(branch, weight_down(j)) * slope).astype(bf16)
                add_vector(6 + j, column_sum(pre_grad.astype(f32)))
                up_sum[j] += dot_tn(normed_low, pre_grad)
                normed_grad = normed_grad + dot_nt(pre_grad, weight_up(j))
            add_vector(2, column_sum(normed_grad * hat))
            add_vector(3, column_sum(normed_grad))
            middle_grad = grad + norm_backward(normed_grad, hat, rho, vector(2))
            carry[rows, :] = middle_grad
            attended = middle_grad.astype(bf16)
            out_sum[...] += dot_tn(mixed[step, rows, :], attended)
            before_out = dot_nt(attended, weight_out()).astype(bf16)
            mixed_grad[rows, :] = before_out
            product = before_out.astype(f32) * mixed[step, rows, :].astype(f32)
            head = jnp.where(iota((HEADS, D), 1) // 64 == iota((HEADS, D), 0), 1.0, 0.0).astype(bf16)
            high = product.astype(bf16)
            centre = dot_nt(head, high) + dot_nt(head, (product - high.astype(f32)).astype(bf16))
            for unit in range(size // UNIT):
                centres[start // UNIT + unit] = centre[:, unit * UNIT : (unit + 1) * UNIT]

        over_rows(query_rows(step), SIZES_BACK, body)

    def attend_back(step):
        inside = iota((SEQ, 1), 0) < length

        def each_pair(pair, carried):
            def lanes(offset):
                return pl.ds(pl.multiple_of(offset + pair * PAIR, PAIR), PAIR)

            def clear(start, size):
                projected_grad[at_rows(start, size), lanes(0)] = jnp.zeros((size, PAIR), bf16)

            key_sum[...] = jnp.zeros_like(key_sum)
            value_sum[...] = jnp.zeros_like(value_sum)
            own_keys = projected[step, :, lanes(D)]
            turned[...] = jnp.where(inside, own_keys, jnp.zeros_like(own_keys)).T

            def body(start, size):
                rows = at_rows(start, size)
                keys, values = projected[step, :, lanes(D)], projected[step, :, lanes(2 * D)]
                queries, grads = projected[step, rows, lanes(0)], mixed_grad[rows, lanes(0)]
                query_half = [jnp.where(o, queries, jnp.zeros_like(queries)) for o in own]
                grad_half = [jnp.where(o, grads, jnp.zeros_like(grads)) for o in own]
                weights, slopes = [], []
                for h in range(2):
                    units = [start // UNIT + unit for unit in range(size // UNIT)]
                    log = jnp.concatenate([logs[step, unit, pl.ds(2 * pair + h, 1), :] for unit in units], axis=1)
                    centre = jnp.concatenate([centres[unit, pl.ds(2 * pair + h, 1), :] for unit in units], axis=1)
                    attention = jnp.exp2(dot_nt(keys, query_half[h]) * SCORE_LOG2 - log)
                    slope = (attention * (dot_nt(values, grad_half[h]) - centre)).astype(bf16)
                    weights.append(attention.astype(bf16))
                    slopes.append(slope)
                value_sum[...] += dot(jnp.concatenate(weights, axis=1), jnp.concatenate(grad_half, axis=0))
                key_sum[...] += dot(jnp.concatenate(slopes, axis=1), jnp.concatenate(query_half, axis=0))
                turned_grads = [dot(turned[64 * h : 64 * (h + 1), :], slopes[h]) for h in range(2)]
                projected_grad[rows, lanes(0)] = (jnp.concatenate(turned_grads, axis=0).T * SCORE_SCALE).astype(bf16)

            covered = over_rows(query_rows(step), SIZES_ATTEND_BACK, body)
            rest_rows(covered, clear)
            projected_grad[:, lanes(D)] = jnp.where(inside, key_sum[...] * SCORE_SCALE, 0.0).astype(bf16)
            projected_grad[:, lanes(2 * D)] = jnp.where(inside, value_sum[...], 0.0).astype(bf16)
            return carried

        lax.fori_loop(0, PAIRS, each_pair, 0)

    def project_back(step):
        def body(start, size):
            rows = at_rows(start, size)
            hat, rho = normalize(state[step, rows, :])
            normed_low = (hat * vector(0) + vector(1)).astype(bf16)
            normed_grad = jnp.zeros((size, D), f32)
            for j in range(3):
                grads = projected_grad[rows, D * j : D * (j + 1)]
                qkv_sum[j] += dot_tn(normed_low, grads)
                normed_grad = normed_grad + dot_nt(grads, weight_qkv(j))
            add_vector(0, column_sum(normed_grad * hat))
            add_vector(1, column_sum(normed_grad))
            through = norm_backward(normed_grad, hat, rho, vector(0))
            direct = jnp.where(step == 1, state[2, rows, :], 0.0)
            carry[rows, :] = jnp.where(row_index(start, size) < length, carry[rows, :] + through + direct, 0.0)

        over_rows(length, SIZES_LENGTH, body)

    def backward(back_step, carried):
        step = 1 - back_step

        @pl.when(step == 0)
        def _():
            fetch().wait()

        feed_back(step)

        @pl.when(step == 1)
        def _():
            fetch().start()

        attend_back(step)
        project_back(step)
        return carried

    lax.fori_loop(0, 2, backward, 0)

    def place(row, rows, value):
        while rows:
            chunk, inside = divmod(row, CHUNK)
            some = min(rows, CHUNK - inside)
            at = PACKED * chunk + inside
            hidden[at : at + some, :] = value[:some]
            value, row, rows = value[some:], row + some, rows - some

    for j in range(3):
        for n in range(8):
            place(CHUNK * n + 64 * j, 64, qkv_sum[j, 64 * n : 64 * (n + 1), :].astype(bf16))
    place(1536, 512, out_sum[...].astype(bf16))
    for j in range(4):
        for at, rows, first in UP_SEGMENTS:
            place(2048 + at + rows * j, rows, up_sum[j, first : first + rows, :].astype(bf16))
        place(4096 + D * j, D, down_sum[j].T.astype(bf16))
    for n in range(DEVICES):
        extra = next_rows(n, qkv_sum, out_sum, up_sum, hidden, vector_sum).astype(bf16)
        hidden[PACKED * n + CHUNK : PACKED * (n + 1), :] = extra
    copies = []
    for dc in range(2):
        part_a, part_b = (keep_a, keep_b) if dc == 0 else (send_a, send_b)
        for plane, (dy, dx) in enumerate(PLANE):
            for dz in range(4):
                row = pl.multiple_of(chunk_of(meta, dy, dc, dz, dx) * PACKED, 16)
                for part, index, first, some in (
                    (part_a, 4 * dz + plane, 0, ROWS_A),
                    (part_b, 4 * plane + dz, ROWS_A, ROWS_B),
                ):
                    copy = pltpu.make_async_copy(
                        hidden.at[pl.ds(row + first, some), :], part.at[index], out_sem.at[len(copies)]
                    )
                    copy.start()
                    copies.append(copy)
    for copy in copies:
        copy.wait()


def layer(meta, states, cotangent, pieces):
    in_place = pl.BlockSpec(memory_space=pltpu.VMEM)
    outside = pl.BlockSpec(memory_space=pl.ANY)
    outputs = pl.pallas_call(
        layer_kernel,
        out_shape=(
            shape_of(SEQ, D),
            shape_of(SEQ, D),
            shape_of(16, ROWS_A, D, dtype=bf16),
            shape_of(16, ROWS_A, D, dtype=bf16),
            shape_of(16, ROWS_B, D, dtype=bf16),
            shape_of(16, ROWS_B, D, dtype=bf16),
            shape_of(8 * SEQ, D, dtype=bf16),
        ),
        in_specs=[pl.BlockSpec(memory_space=pltpu.SMEM)] + [in_place] * 2 + [outside] * 16,
        out_specs=(in_place, in_place) + (outside,) * 5,
        scratch_shapes=[
            pltpu.VMEM((DEVICES * CHUNK, D), bf16),
            pltpu.VMEM((DEVICES, EXTRA, D), bf16),
            pltpu.VMEM((EXTRA, D), f32),
            pltpu.VMEM((3, SEQ, D), f32),
            pltpu.VMEM((2, SEQ, 3 * D), bf16),
            pltpu.VMEM((2, SEQ, D), bf16),
            pltpu.VMEM((2, SEQ, D), f32),
            pltpu.VMEM((8 * SEQ, D), bf16),
            pltpu.VMEM((SEQ, D), bf16),
            pltpu.VMEM((SEQ, 3 * D), bf16),
            pltpu.VMEM((2, SEQ // UNIT, HEADS, UNIT), f32),
            pltpu.VMEM((SEQ // UNIT, HEADS, UNIT), f32),
            pltpu.VMEM((3, D, D), f32),
            pltpu.VMEM((D, D), f32),
            pltpu.VMEM((4, D, D), f32),
            pltpu.VMEM((4, D, D), f32),
            pltpu.VMEM((16, D), f32),
            pltpu.VMEM((8, D), f32),
            pltpu.VMEM((8, PAIR), f32),
            pltpu.VMEM((SEQ, PAIR), f32),
            pltpu.VMEM((SEQ, PAIR), f32),
            pltpu.VMEM((PAIR, SEQ), bf16),
            pltpu.SemaphoreType.DMA((96,)),
            pltpu.SemaphoreType.DMA,
            pltpu.SemaphoreType.DMA((64,)),
        ],
        compiler_params=pltpu.CompilerParams(vmem_limit_bytes=63 * 1024 * 1024),
        name="layer",
    )(meta, states, cotangent, *pieces)
    return outputs[0], outputs[1], outputs[2:6]


def to_chunks(flat):
    wide = flat[:QKV_END].reshape(8, 64, 3, D).transpose(0, 2, 1, 3).reshape(1536, D)
    up = flat[OUT_END:UP_END].reshape(512, 4, D)
    pieces = [up[first : first + rows].transpose(1, 0, 2).reshape(4 * rows, D) for _, rows, first in UP_SEGMENTS]
    return jnp.concatenate(
        [wide, flat[QKV_END:OUT_END].reshape(D, D), *pieces, flat[UP_END:DOWN_END].reshape(FF, D)], axis=0
    )


def from_chunks(rows):
    wide = rows[:1536].reshape(8, 3, 64, D).transpose(0, 2, 1, 3).reshape(-1)
    up = rows[2048:4096]
    pieces = [
        up[at : at + 4 * rows].reshape(4, rows, D).transpose(1, 0, 2).reshape(-1) for at, rows, _ in UP_SEGMENTS
    ]
    return jnp.concatenate([wide, rows[1536:2048].reshape(-1), *pieces, rows[4096:].reshape(-1)])


def row_tables():
    order = np.concatenate(
        [
            (np.arange(1536).reshape(8, 64, 3).transpose(0, 2, 1)).reshape(-1),
            np.arange(1536, 2048),
            *[
                2048 + 4 * first + np.arange(4 * rows).reshape(rows, 4).transpose(1, 0).reshape(-1)
                for _, rows, first in UP_SEGMENTS
            ],
            np.arange(4096, 6144),
        ]
    )
    source = np.full((DEVICES, CHUNK + EXTRA), -1, np.int32)
    target = np.tile(np.arange(CHUNK + EXTRA, dtype=np.int32), (DEVICES, 1))
    for n in range(DEVICES):
        source[n, :CHUNK] = order[CHUNK * n : CHUNK * (n + 1)] - CHUNK * n
        target[n, source[n, :CHUNK]] = np.arange(CHUNK)
        width = 3 if n + 1 < 8 else 4 if 11 <= n + 1 < 22 else 1
        for row in range(10):
            at = row if width == 1 else 4 * (row % width) + row // width
            source[n, CHUNK + at] = CHUNK + row
    return source, target


def pick_rows(table, device, rows, precision=None):
    wanted = lax.dynamic_slice(jnp.asarray(table), (device, 0), (1, CHUNK + EXTRA)).reshape(-1, 1)
    pick = (wanted == iota((CHUNK + EXTRA, CHUNK + EXTRA), 1)).astype(rows.dtype)
    return jnp.dot(pick, rows, precision=precision, preferred_element_type=f32)


def send(array, dy=0, dx=0, dz=0, dc=0):
    pairs = []
    for y in range(2):
        for c in range(2):
            for z in range(4):
                for x in range(2):
                    other = (((y ^ dy) * 2 + (c ^ dc)) * 4 + (z ^ dz)) * 2 + (x ^ dx)
                    pairs.append((((y * 2 + c) * 4 + z) * 2 + x, other))
    return lax.ppermute(array, ("dp", "fsdp"), pairs)


def gather_weights(params, device, meanwhile):
    source, _ = row_tables()
    shift = (NPARAM // DEVICES - CHUNK * D) * device
    edge = jnp.zeros((EXTRA * D,), bf16)
    line = jnp.concatenate([edge, params.astype(bf16), edge])
    rows = lax.dynamic_slice(line, (EXTRA * D - shift,), ((CHUNK + EXTRA) * D,)).reshape(CHUNK + EXTRA, D)
    rows = pick_rows(source, device, rows).astype(bf16)
    own_a, own_b = rows[:ROWS_A], rows[ROWS_A:]
    first_a = jnp.stack([own_a] + [send(own_a, dy, dx) for dy, dx in PLANE[1:]])
    first_b = jnp.stack([own_b] + [send(own_b, dz=dz) for dz in (1, 2, 3)])
    first_a, first_b, meanwhile = lax.optimization_barrier((first_a, first_b, meanwhile))
    all_b = [first_b] + [send(first_b, dy, dx) for dy, dx in PLANE[1:]]
    all_a = [first_a] + [send(first_a, dz=dz) for dz in (1, 2, 3)]
    other_a = [send(part, dc=1) for part in all_a]
    other_b = [send(part, dc=1) for part in all_b]
    return all_a + other_a + all_b + other_b, meanwhile


def cut_weights(flat):
    chunks = to_chunks(flat[:DOWN_END]).reshape(DEVICES, CHUNK, D)
    extra = jnp.zeros((DEVICES, EXTRA, D), bf16).at[DEVICES - 1, :10].set(flat[DOWN_END:].reshape(10, D))
    chunks = jnp.concatenate([chunks, extra], axis=1).reshape(2, 2, 4, 2, PACKED, D)
    parts_a = chunks[..., :ROWS_A, :].transpose(1, 2, 3, 0, 4, 5).reshape(8, 4, ROWS_A, D)
    parts_b = chunks[..., ROWS_A:, :].transpose(1, 3, 0, 2, 4, 5).reshape(8, 4, ROWS_B, D)
    return [parts_a[n] for n in range(8)] + [parts_b[n] for n in range(8)]


def reduce_grads(parts, device, place, final_states, input_grad):
    keep_a, send_a, keep_b, send_b = parts
    _, target = row_tables()
    core_b, core_a = send(send_b, dc=1), send(send_a, dc=1)
    final_states = restore(place, final_states, "restore_final")
    core_a, final_states = lax.optimization_barrier((core_a, final_states))
    pair_a = [keep_a[4 * n : 4 * n + 4] + core_a[4 * n : 4 * n + 4] for n in range(4)]
    pair_b = [keep_b[4 * n : 4 * n + 4] + core_b[4 * n : 4 * n + 4] for n in range(4)]
    got_a = [send(pair_a[dz], dz=dz) for dz in (1, 2, 3)]
    got_b = [send(pair_b[n], *PLANE[n]) for n in (1, 2, 3)]
    line_a = sum((part.astype(f32) for part in got_a), pair_a[0].astype(f32))
    plane_b = sum((part.astype(f32) for part in got_b), pair_b[0].astype(f32))
    line_a, plane_b, input_grad = lax.optimization_barrier((line_a, plane_b, input_grad))
    got_b = [send(plane_b[dz].astype(bf16), dz=dz) for dz in (1, 2, 3)]
    got_a = [send(line_a[n].astype(bf16), *PLANE[n]) for n in (1, 2, 3)]
    input_grad = restore(place, input_grad, "restore_grad")
    got_a, got_b, input_grad = lax.optimization_barrier((got_a, got_b, input_grad))
    own_a = sum((part.astype(f32) for part in got_a), line_a[0])
    own_b = sum((part.astype(f32) for part in got_b), plane_b[0])
    rows = pick_rows(target, device, jnp.concatenate([own_a, own_b], axis=0), lax.Precision.HIGHEST)
    shift = (NPARAM // DEVICES - CHUNK * D) * device
    return lax.dynamic_slice(rows.reshape(-1), (shift,), (NPARAM // DEVICES,)), final_states, input_grad


def sum_all(value):
    value = jnp.broadcast_to(value, (8, 128))
    value = value + send(value, dc=1)
    value = value + sum(send(value, dy, dx) for dy, dx in PLANE[1:])
    return (value + sum(send(value, dz=dz) for dz in (1, 2, 3)))[0, 0]


def flat_grads(parts):
    keep_a, send_a, keep_b, send_b = parts
    chunks_a = jnp.stack([keep_a, send_a]).reshape(2, 4, 2, 2, ROWS_A, D).transpose(3, 0, 1, 2, 4, 5)
    chunks_b = jnp.stack([keep_b, send_b]).reshape(2, 2, 2, 4, ROWS_B, D).transpose(2, 0, 3, 1, 4, 5)
    chunks = jnp.concatenate(
        [chunks_a.reshape(DEVICES, ROWS_A, D), chunks_b.reshape(DEVICES, ROWS_B, D)], axis=1
    )
    rows = chunks[:, :CHUNK].reshape(DEVICES * CHUNK, D)
    vectors = chunks[DEVICES - 1, CHUNK : CHUNK + 10].reshape(-1)
    return jnp.concatenate([from_chunks(rows), vectors]).astype(f32)


def local(ways, states, params, first_moment, second_moment, ema_params, lengths, halt_counts, cotangent):
    both = ("dp", "fsdp")
    device = lax.axis_index(both)
    blockwise = ways == (4, 8)
    if blockwise:
        outer, inner = lax.axis_index("dp"), lax.axis_index("fsdp")
        place_index = jnp.stack([outer // 2, outer % 2, inner // 2, inner % 2]).astype(i32)
    else:
        place_index = jnp.zeros((4,), i32)
    prepared = prepare(lengths, place_index, halt_counts, states[0], cotangent[0])
    if blockwise:
        pieces, prepared = gather_weights(params, device, prepared)
    else:
        pieces = cut_weights(lax.all_gather(params.astype(bf16), both, axis=0, tiled=True))
    place, sorted_states, sorted_cotangent, meta = prepared
    final_states, input_grad, parts = layer(meta, sorted_states, sorted_cotangent, pieces)
    if blockwise:
        reduced, final_states, input_grad = reduce_grads(parts, device, place, final_states, input_grad)
        square_sum = sum_all(jnp.sum(reduced * reduced))
    else:
        final_states = restore(place, final_states, "restore_final")
        input_grad = restore(place, input_grad, "restore_grad")
        reduced = lax.psum_scatter(flat_grads(parts), both, scatter_dimension=0, tiled=True)
        square_sum = lax.psum(jnp.sum(reduced * reduced), both)
    grad_norm = jnp.sqrt(square_sum)
    clip_bound = NPARAM**0.5
    clipped = reduced * (clip_bound / jnp.maximum(grad_norm, clip_bound))
    new_first = BETA_FIRST * first_moment + (1.0 - BETA_FIRST) * clipped
    new_second = BETA_SECOND * second_moment + (1.0 - BETA_SECOND) * clipped * clipped
    first_hat = new_first / (1.0 - BETA_FIRST**ADAM_STEP)
    second_hat = new_second / (1.0 - BETA_SECOND**ADAM_STEP)
    shard_length = params.shape[0]
    index_all = device * shard_length + iota((shard_length,), 0)
    matrix = index_all < DOWN_END
    step_rate = jnp.where(matrix, RATE_MATRIX, RATE_VECTOR)
    decay_rate = jnp.where(matrix, WEIGHT_DECAY, 0.0)
    new_params = params - step_rate * (first_hat / (jnp.sqrt(second_hat) + ADAM_EPSILON) + decay_rate * params)
    average_decay = min(EMA_DECAY, (1.0 + ADAM_STEP) / (10.0 + ADAM_STEP))
    new_ema = average_decay * ema_params + (1.0 - average_decay) * new_params
    return (
        final_states[None],
        input_grad[None],
        clipped,
        grad_norm.reshape(1),
        new_params,
        new_first,
        new_second,
        new_ema,
        new_params.astype(bf16),
    )


def solution(mesh):
    both = ("dp", "fsdp")
    wide, flat, counts = P(both, None, None), P(both), P(both, None)
    ways = (mesh.shape["dp"], mesh.shape["fsdp"])
    return jax.shard_map(
        functools.partial(local, ways),
        mesh=mesh,
        in_specs=(wide, flat, flat, flat, flat, flat, counts, wide),
        out_specs=(wide, wide, flat, P(), flat, flat, flat, flat, flat),
        check_vma=False,
    )
```

```python
import functools
import math

import jax
import jax.numpy as jnp
import numpy as np
from jax import lax
from jax.experimental import pallas as pl
from jax.experimental.pallas import tpu as pltpu
from jax.sharding import PartitionSpec as P

D = 512
FF = 2048
HEADS = 8
SEQ = 1024
ADAM_STEP = 4
QKV_END = 786432
OUT_END = 1048576
UP_END = 2097152
DOWN_END = 3145728
NPARAM = 3150848

NORM_EPSILON = 1e-05
HALT_SHIFT = -1.0
BETA_FIRST = 0.9
BETA_SECOND = 0.999
ADAM_EPSILON = 1e-08
EMA_DECAY = 0.999
WEIGHT_DECAY = 0.1
RATE_MATRIX = 0.1
RATE_VECTOR = 1.0

BLOCK = 256
BLOCKS = SEQ // BLOCK
UNIT = 128
SIZES_LENGTH = (512,)
SIZES_ATTEND = (256, 128)
SIZES_SHIFTED = (128,)
SIZES_ATTEND_BACK = (256,)
SIZES_FEED = (512, 128)
SIZES_BACK = (512, 128)
PAIRS = HEADS // 2
PAIR = 128
SCORE_SCALE = 0.125
SCORE_LOG2 = SCORE_SCALE * math.log2(math.e)

f32 = jnp.float32
bf16 = jnp.bfloat16
i32 = jnp.int32

CHUNK = 192
DEVICES = 32
ROWS_A = 64
ROWS_B = 144
EXTRA = 16
PACKED = CHUNK + EXTRA
PLANE = [(0, 0), (1, 0), (0, 1), (1, 1)]
UP_SEGMENTS = [(0, 16, 0)] + [(64 + CHUNK * n, 48, 16 + 48 * n) for n in range(10)] + [(64 + CHUNK * 10, 16, 496)]


def dot(left, right):
    return jnp.dot(left, right, preferred_element_type=f32)


def dot_nt(left, right):
    return lax.dot_general(left, right, (((1,), (1,)), ((), ())), preferred_element_type=f32)


def dot_tn(left, right):
    return lax.dot_general(left, right, (((0,), (0,)), ((), ())), preferred_element_type=f32)


def iota(shape, axis):
    return lax.broadcasted_iota(i32, shape, axis)


def normalize(inputs):
    centred = inputs - jnp.mean(inputs, axis=-1, keepdims=True)
    rho = lax.rsqrt(jnp.mean(centred * centred, axis=-1, keepdims=True) + NORM_EPSILON)
    return centred * rho, rho


def norm_backward(grad_out, hat, rho, gain):
    grad_hat = grad_out * gain
    return rho * (
        grad_hat
        - jnp.mean(grad_hat, axis=-1, keepdims=True)
        - hat * jnp.mean(grad_hat * hat, axis=-1, keepdims=True)
    )


def gelu_parts(pre):
    cumulative = 0.5 + 0.5 * lax.erf(pre * 0.7071067811865476)
    density = jnp.exp2(pre * pre * (-0.5 * math.log2(math.e))) * 0.3989422804014327
    return pre * cumulative, cumulative + pre * density


def qkv_weight(ref, j):
    return jnp.concatenate([ref[CHUNK * n + 64 * j : CHUNK * n + 64 * (j + 1), :] for n in range(8)], axis=0)


def up_weight(ref, j):
    return jnp.concatenate(
        [ref[2048 + at + rows * j : 2048 + at + rows * (j + 1), :] for at, rows, _ in UP_SEGMENTS], axis=0
    )


def prepare_kernel(
    length_ref, index_ref, count_ref, state_ref, cotangent_ref, place_ref, states_out, cotangent_out, meta_ref
):
    length = length_ref[0]
    token = iota((1, SEQ), 1)
    valid = token < length
    two = jnp.where(valid & (count_ref[...] >= 2), 1.0, 0.0)
    one = jnp.where(valid & (count_ref[...] < 2), 1.0, 0.0)
    masks = jnp.concatenate([two, one, jnp.zeros((6, SEQ), f32)], axis=0).astype(bf16)
    earlier = jnp.where(iota((SEQ, SEQ), 0) < iota((SEQ, SEQ), 1), 1.0, 0.0).astype(bf16)
    ranks = dot(masks, earlier)
    n_two = jnp.sum(two)
    place = jnp.where(
        two > 0.0, ranks[0:1, :], jnp.where(one > 0.0, n_two + ranks[1:2, :], token.astype(f32))
    )
    place_ref[...] = jnp.broadcast_to(place, (8, SEQ))
    meta_ref[0] = n_two.astype(i32)
    meta_ref[1] = length
    for n in range(4):
        meta_ref[2 + n] = index_ref[n]

    def sort(block, carried):
        rows = pl.ds(pl.multiple_of(block * BLOCK, BLOCK), BLOCK)
        pick = jnp.where((iota((BLOCK, SEQ), 0) + block * BLOCK).astype(f32) == place, 1.0, 0.0).astype(bf16)
        states_out[rows, :] = dot(pick, state_ref[...]).astype(bf16)
        cotangent_out[rows, :] = dot(pick, cotangent_ref[...]).astype(bf16)
        return carried

    lax.fori_loop(0, BLOCKS, sort, 0)


def prepare(lengths, place_index, counts, states, cotangent):
    return pl.pallas_call(
        prepare_kernel,
        out_shape=(
            jax.ShapeDtypeStruct((8, SEQ), f32),
            jax.ShapeDtypeStruct((SEQ, D), bf16),
            jax.ShapeDtypeStruct((SEQ, D), bf16),
            jax.ShapeDtypeStruct((6,), i32),
        ),
        in_specs=[
            pl.BlockSpec(memory_space=pltpu.SMEM),
            pl.BlockSpec(memory_space=pltpu.SMEM),
            pl.BlockSpec(memory_space=pltpu.VMEM),
            pl.BlockSpec(memory_space=pltpu.VMEM),
            pl.BlockSpec(memory_space=pltpu.VMEM),
        ],
        out_specs=(
            pl.BlockSpec(memory_space=pltpu.VMEM),
            pl.BlockSpec(memory_space=pltpu.VMEM),
            pl.BlockSpec(memory_space=pltpu.VMEM),
            pl.BlockSpec(memory_space=pltpu.SMEM),
        ),
        cost_estimate=pl.CostEstimate(flops=6 * 10**9, transcendentals=0, bytes_accessed=4 * 10**6),
        name="prepare",
    )(lengths, place_index, counts, states, cotangent)


def restore_kernel(place_ref, sorted_ref, out_ref, columns, high, lower):
    columns[...] = jnp.broadcast_to(place_ref[0:1, :], (PAIR, SEQ)).T
    high[...] = sorted_ref[...].astype(bf16)
    lower[...] = (sorted_ref[...] - high[...].astype(f32)).astype(bf16)

    def unsort(block, carried):
        rows = pl.ds(pl.multiple_of(block * BLOCK, BLOCK), BLOCK)
        pick = jnp.concatenate(
            [
                jnp.where(columns[rows, :] == (iota((BLOCK, PAIR), 1) + PAIR * n).astype(f32), 1.0, 0.0).astype(bf16)
                for n in range(SEQ // PAIR)
            ],
            axis=1,
        )
        out_ref[rows, :] = dot(pick, high[...]) + dot(pick, lower[...])
        return carried

    lax.fori_loop(0, BLOCKS, unsort, 0)


def restore(place, array, name):
    return pl.pallas_call(
        restore_kernel,
        out_shape=jax.ShapeDtypeStruct((SEQ, D), f32),
        in_specs=[pl.BlockSpec(memory_space=pltpu.VMEM)] * 2,
        out_specs=pl.BlockSpec(memory_space=pltpu.VMEM),
        scratch_shapes=[pltpu.VMEM((SEQ, PAIR), f32), pltpu.VMEM((SEQ, D), bf16), pltpu.VMEM((SEQ, D), bf16)],
        cost_estimate=pl.CostEstimate(flops=6 * 10**9, transcendentals=0, bytes_accessed=4 * 10**6),
        name=name,
    )(place, array)


def next_rows(chunk, qkv_sum, out_sum, up_sum, packed, vector_sum):
    after = chunk + 1
    if after == DEVICES:
        return vector_sum[...]
    if after < 8:
        blocks = [qkv_sum[j, 64 * after : 64 * after + 8, :] for j in range(3)]
    elif after < 11:
        at = CHUNK * after - 1536
        return out_sum[at : at + 16, :]
    elif after < 22:
        first = 16 + 48 * (after - 11)
        blocks = [up_sum[j, first : first + 8, :] for j in range(4)]
    else:
        return packed[PACKED * after : PACKED * after + 16, :].astype(f32)
    width = len(blocks)
    rows = [blocks[r % width][r // width : r // width + 1, :] for r in range(10)]
    return jnp.concatenate(rows + [jnp.zeros((6, D), f32)], axis=0)


def chunk_of(meta, dy, dc, dz, dx):
    return (((meta[2] ^ dy) * 2 + (meta[3] ^ dc)) * 4 + (meta[4] ^ dz)) * 2 + (meta[5] ^ dx)


def shape_of(*shape, dtype=f32):
    return jax.ShapeDtypeStruct(shape, dtype)


def column_sum(array):
    return jnp.sum(array, axis=0, keepdims=True)


def layer_kernel(meta, states_ref, cotangent_ref, *refs):
    pieces = refs[:16]
    (
        final_out, carry, keep_a, send_a, keep_b, send_b, spill,
        matrices, extras, vectors,
        state, projected, mixed, middle, hidden, mixed_grad, projected_grad, logs, centres,
        qkv_sum, out_sum, up_sum, down_sum, vector_sum, first_key, norm_peak, key_sum, value_sum, turned, in_sem, spill_sem, out_sem,
    ) = refs[16:]
    n_two, length = meta[0], meta[1]
    lower = iota((1, PAIR), 1) < 64
    own = [lower, ~lower]

    def at_rows(start, size):
        return pl.ds(pl.multiple_of(start, UNIT), size)

    def hidden_rows(j, start, size):
        return pl.ds(pl.multiple_of(j * SEQ + start, UNIT), size)

    def over_rows(rows, sizes, body):
        def loop(first, size, count):
            def step(n, carried):
                body(first + n * size, size)
                return carried

            lax.fori_loop(0, count, step, 0)
            return first + count * size

        large = sizes[0]
        if len(sizes) == 1:
            return loop(0, large, (rows + large - 1) // large)
        covered = loop(0, large, (rows + large // 2 - 1) // large)
        return loop(covered, sizes[1], (jnp.maximum(rows - covered, 0) + sizes[1] - 1) // sizes[1])

    def rest_rows(covered, body):
        def step(n, carried):
            body(n * UNIT, UNIT)
            return carried

        lax.fori_loop(covered // UNIT, SEQ // UNIT, step, 0)

    def weight_qkv(j):
        return qkv_weight(matrices, j)

    def weight_out():
        return matrices[1536:2048, :]

    def weight_up(j):
        return up_weight(matrices, j)

    def weight_down(j):
        return matrices[4096 + D * j : 4096 + D * (j + 1), :]

    def vector(index):
        return vectors[index : index + 1, :]

    def add_vector(index, value):
        vector_sum[index : index + 1, :] += value

    def query_rows(step):
        return jnp.where(step == 0, length, n_two)

    def row_index(start, size):
        return iota((size, 1), 0) + start

    arriving = []
    for dc in range(2):
        for plane, (dy, dx) in enumerate(PLANE):
            for dz in range(4):
                chunk = chunk_of(meta, dy, dc, dz, dx)
                row = pl.multiple_of(chunk * CHUNK, CHUNK)
                part_a, part_b = pieces[4 * dc + dz].at[plane], pieces[8 + 4 * dc + plane].at[dz]
                for source, target in (
                    (part_a, matrices.at[pl.ds(row, ROWS_A), :]),
                    (part_b.at[: CHUNK - ROWS_A, :], matrices.at[pl.ds(row + ROWS_A, CHUNK - ROWS_A), :]),
                    (part_b.at[CHUNK - ROWS_A :, :], extras.at[chunk]),
                ):
                    copy = pltpu.make_async_copy(source, target, in_sem.at[len(arriving)])
                    copy.start()
                    arriving.append(copy)

    def start_rows(n, carried):
        rows = at_rows(n * UNIT, UNIT)
        state[0, rows, :] = states_ref[rows, :].astype(f32)
        state[1, rows, :] = jnp.zeros((UNIT, D), f32)
        mixed[0, rows, :] = jnp.zeros((UNIT, D), bf16)
        mixed[1, rows, :] = jnp.zeros((UNIT, D), bf16)
        mixed_grad[rows, :] = jnp.zeros((UNIT, D), bf16)
        return carried

    lax.fori_loop(0, SEQ // UNIT, start_rows, 0)

    def start_sums(n, carried):
        rows = at_rows(n * UNIT, UNIT)
        for total in (qkv_sum, up_sum, down_sum):
            for j in range(total.shape[0]):
                total[j, rows, :] = jnp.zeros((UNIT, D), f32)
        out_sum[rows, :] = jnp.zeros((UNIT, D), f32)
        return carried

    lax.fori_loop(0, D // UNIT, start_sums, 0)
    vector_sum[...] = jnp.zeros_like(vector_sum)
    centres[...] = jnp.zeros_like(centres)
    logs[...] = jnp.full_like(logs, 1e30)
    for copy in arriving:
        copy.wait()

    def complete(row, value):
        rows = value.shape[0]
        matrices[row : row + rows, :] = (matrices[row : row + rows, :].astype(f32) + value).astype(bf16)

    for n in range(1, DEVICES):
        value = extras[n - 1].astype(f32)
        if n < 8 or 11 <= n < 22:
            width, stride = (3, 64) if n < 8 else (4, 48 if n < 21 else 16)
            for j in range(width):
                rows = jnp.concatenate([value[4 * j : 4 * j + 4, :], jnp.zeros((4, D), f32)], axis=0)
                complete(CHUNK * n + stride * j, rows)
        else:
            complete(CHUNK * n, value)
    vectors[...] = extras[DEVICES - 1].astype(f32)

    heads = jnp.where(iota((D, PAIR), 0) // 64 == iota((D, PAIR), 1), 1.0, 0.0).astype(bf16)

    def project(step):
        def body(start, size):
            rows = at_rows(start, size)
            hat, _ = normalize(state[step, rows, :])
            normed_low = (hat * vector(0) + vector(1)).astype(bf16)
            queries = dot(normed_low, weight_qkv(0))
            projected[step, rows, 0:D] = queries.astype(bf16)
            keys = dot(normed_low, weight_qkv(1))
            for index, array in enumerate((queries, keys)):
                norms = dot((array * array).astype(bf16), heads)
                norm_peak[index : index + 1, :] = jnp.maximum(
                    norm_peak[index : index + 1, :], jnp.max(norms, axis=0, keepdims=True)
                )

            @pl.when(start == 0)
            def _():
                first_key[...] = jnp.broadcast_to(keys[0:1, :], first_key.shape)

            inside = row_index(start, size) < length
            projected[step, rows, D : 2 * D] = jnp.where(inside, keys, first_key[0:1, :]).astype(bf16)
            values = dot(normed_low, weight_qkv(2))
            projected[step, rows, 2 * D : 3 * D] = jnp.where(inside, values, 0.0).astype(bf16)

        def fill(start, size):
            rows = at_rows(start, size)
            projected[step, rows, D : 2 * D] = jnp.broadcast_to(first_key[0:1, :], (size, D)).astype(bf16)
            projected[step, rows, 2 * D : 3 * D] = jnp.zeros((size, D), bf16)

        norm_peak[...] = jnp.zeros_like(norm_peak)
        rest_rows(over_rows(length, SIZES_LENGTH, body), fill)

    def attend_pair(step, start, size, pair, shifted):
        rows = at_rows(start, size)
        ones = jnp.where(iota((SEQ, 1), 0) < length, 1.0, 0.0).astype(bf16)
        def lanes(offset):
            at = offset + pair * PAIR
            return pl.ds(at if isinstance(at, int) else pl.multiple_of(at, PAIR), PAIR)

        queries = projected[step, rows, lanes(0)]
        keys = projected[step, :, lanes(D)]
        values = projected[step, :, lanes(2 * D)]
        peaks, sums = [], []
        for half in range(2):
            scores = dot_nt(jnp.where(own[half], queries, jnp.zeros_like(queries)), keys) * SCORE_LOG2
            if shifted:
                peaks.append(jnp.max(scores, axis=-1, keepdims=True))
                scores = scores - peaks[half]
            sums.append(dot(jnp.exp2(scores).astype(bf16), jnp.where(own[half], values, ones)))
        total = jnp.where(lower, pltpu.roll(sums[0], 64, 1), pltpu.roll(sums[1], 64, 1))
        mixed[step, rows, lanes(0)] = (jnp.where(lower, sums[0], sums[1]) / total).astype(bf16)
        log = jnp.log2(total)
        if shifted:
            log = log + jnp.where(lower, peaks[0], peaks[1])
        log = log.T
        for unit in range(size // UNIT):
            columns = slice(unit * UNIT, (unit + 1) * UNIT)
            logs[step, start // UNIT + unit, pl.ds(2 * pair, 1), :] = log[0:1, columns]
            logs[step, start // UNIT + unit, pl.ds(2 * pair + 1, 1), :] = log[64:65, columns]

    def attend(step):
        bound = jnp.max(norm_peak[0:1, :] * norm_peak[1:2, :])
        plain = bound * (1.02 * SCORE_LOG2) ** 2 < 60.0**2

        @pl.when(plain)
        def _():
            def body(start, size):
                def each(pair, carried):
                    attend_pair(step, start, size, pair, False)
                    return carried

                if size == SIZES_ATTEND[0]:
                    for pair in range(PAIRS):
                        each(pair, 0)
                else:
                    lax.fori_loop(0, PAIRS, each, 0)

            over_rows(query_rows(step), SIZES_ATTEND, body)

        @pl.when(~plain)
        def _():
            def body(start, size):
                def each(pair, carried):
                    attend_pair(step, start, size, pair, True)
                    return carried

                lax.fori_loop(0, PAIRS, each, 0)

            over_rows(query_rows(step), SIZES_SHIFTED, body)

    def feed_forward(step):
        def body(start, size):
            rows = at_rows(start, size)
            between = state[step, rows, :] + dot(mixed[step, rows, :], weight_out())
            middle[step, rows, :] = between
            hat, _ = normalize(between)
            normed_low = (hat * vector(2) + vector(3)).astype(bf16)
            output = between + vector(4)
            for j in range(4):
                value, slope = gelu_parts(dot(normed_low, weight_up(j)) + vector(6 + j))
                value_low = value.astype(bf16)
                hidden[hidden_rows(j, start, size), :] = value_low
                hidden[hidden_rows(4 + j, start, size), :] = slope.astype(bf16)
                output = output + dot(value_low, weight_down(j))
            state[step + 1, rows, :] = output

        over_rows(query_rows(step), SIZES_FEED, body)

    def save():
        return pltpu.make_async_copy(hidden, spill, spill_sem)

    def fetch():
        return pltpu.make_async_copy(spill, hidden, spill_sem)

    def forward(step, carried):
        project(step)
        attend(step)

        @pl.when(step == 1)
        def _():
            save().wait()

        feed_forward(step)

        @pl.when(step == 0)
        def _():
            save().start()

        return carried

    lax.fori_loop(0, 2, forward, 0)

    def mix(start, size):
        rows = at_rows(start, size)
        row = row_index(start, size)
        two, valid = row < n_two, row < length
        before = state[1, rows, :]
        after = jnp.where(two, state[2, rows, :], before)
        halting = jax.nn.sigmoid(jnp.sum(before * vector(5), axis=-1, keepdims=True) + HALT_SHIFT)
        share_one = jnp.where(two, halting, 1.0)
        share_two = jnp.where(two, 1.0 - halting, 0.0)
        final_out[rows, :] = jnp.where(valid, share_one * before + share_two * after, 0.0)
        grad_final = jnp.where(valid, cotangent_ref[rows, :].astype(f32), 0.0)
        first_sum = jnp.sum(grad_final * before, axis=-1, keepdims=True)
        second_sum = jnp.sum(grad_final * after, axis=-1, keepdims=True)
        logit_grad = jnp.where(two, (first_sum - second_sum) * halting * (1.0 - halting), 0.0)
        add_vector(5, column_sum(jnp.where(valid, logit_grad * before, 0.0)))
        carry[rows, :] = share_two * grad_final
        state[2, rows, :] = jnp.where(valid, share_one * grad_final + logit_grad * vector(5), 0.0)

    def blank(start, size):
        rows = at_rows(start, size)
        final_out[rows, :] = jnp.zeros((size, D), f32)
        carry[rows, :] = jnp.zeros((size, D), f32)

    rest_rows(over_rows(length, SIZES_LENGTH, mix), blank)

    def feed_back(step):
        def body(start, size):
            rows = at_rows(start, size)
            grad = carry[rows, :]
            branch = grad.astype(bf16)
            add_vector(4, column_sum(branch.astype(f32)))
            hat, rho = normalize(middle[step, rows, :])
            normed_low = (hat * vector(2) + vector(3)).astype(bf16)
            normed_grad = jnp.zeros((size, D), f32)
            for j in range(4):
                down_sum[j] += dot_tn(branch, hidden[hidden_rows(j, start, size), :])
                slope = hidden[hidden_rows(4 + j, start, size), :].astype(f32)
                pre_grad = (dot_nt(branch, weight_down(j)) * slope).astype(bf16)
                add_vector(6 + j, column_sum(pre_grad.astype(f32)))
                up_sum[j] += dot_tn(normed_low, pre_grad)
                normed_grad = normed_grad + dot_nt(pre_grad, weight_up(j))
            add_vector(2, column_sum(normed_grad * hat))
            add_vector(3, column_sum(normed_grad))
            middle_grad = grad + norm_backward(normed_grad, hat, rho, vector(2))
            carry[rows, :] = middle_grad
            attended = middle_grad.astype(bf16)
            out_sum[...] += dot_tn(mixed[step, rows, :], attended)
            before_out = dot_nt(attended, weight_out()).astype(bf16)
            mixed_grad[rows, :] = before_out
            product = before_out.astype(f32) * mixed[step, rows, :].astype(f32)
            head = jnp.where(iota((HEADS, D), 1) // 64 == iota((HEADS, D), 0), 1.0, 0.0).astype(bf16)
            high = product.astype(bf16)
            centre = dot_nt(head, high) + dot_nt(head, (product - high.astype(f32)).astype(bf16))
            for unit in range(size // UNIT):
                centres[start // UNIT + unit] = centre[:, unit * UNIT : (unit + 1) * UNIT]

        over_rows(query_rows(step), SIZES_BACK, body)

    def attend_back(step):
        inside = iota((SEQ, 1), 0) < length

        def each_pair(pair, carried):
            def lanes(offset):
                return pl.ds(pl.multiple_of(offset + pair * PAIR, PAIR), PAIR)

            def clear(start, size):
                projected_grad[at_rows(start, size), lanes(0)] = jnp.zeros((size, PAIR), bf16)

            key_sum[...] = jnp.zeros_like(key_sum)
            value_sum[...] = jnp.zeros_like(value_sum)
            own_keys = projected[step, :, lanes(D)]
            turned[...] = jnp.where(inside, own_keys, jnp.zeros_like(own_keys)).T

            def body(start, size):
                rows = at_rows(start, size)
                keys, values = projected[step, :, lanes(D)], projected[step, :, lanes(2 * D)]
                queries, grads = projected[step, rows, lanes(0)], mixed_grad[rows, lanes(0)]
                query_half = [jnp.where(o, queries, jnp.zeros_like(queries)) for o in own]
                grad_half = [jnp.where(o, grads, jnp.zeros_like(grads)) for o in own]
                weights, slopes = [], []
                for h in range(2):
                    units = [start // UNIT + unit for unit in range(size // UNIT)]
                    log = jnp.concatenate([logs[step, unit, pl.ds(2 * pair + h, 1), :] for unit in units], axis=1)
                    centre = jnp.concatenate([centres[unit, pl.ds(2 * pair + h, 1), :] for unit in units], axis=1)
                    attention = jnp.exp2(dot_nt(keys, query_half[h]) * SCORE_LOG2 - log)
                    slope = (attention * (dot_nt(values, grad_half[h]) - centre)).astype(bf16)
                    weights.append(attention.astype(bf16))
                    slopes.append(slope)
                value_sum[...] += dot(jnp.concatenate(weights, axis=1), jnp.concatenate(grad_half, axis=0))
                key_sum[...] += dot(jnp.concatenate(slopes, axis=1), jnp.concatenate(query_half, axis=0))
                turned_grads = [dot(turned[64 * h : 64 * (h + 1), :], slopes[h]) for h in range(2)]
                projected_grad[rows, lanes(0)] = (jnp.concatenate(turned_grads, axis=0).T * SCORE_SCALE).astype(bf16)

            covered = over_rows(query_rows(step), SIZES_ATTEND_BACK, body)
            rest_rows(covered, clear)
            projected_grad[:, lanes(D)] = jnp.where(inside, key_sum[...] * SCORE_SCALE, 0.0).astype(bf16)
            projected_grad[:, lanes(2 * D)] = jnp.where(inside, value_sum[...], 0.0).astype(bf16)
            return carried

        lax.fori_loop(0, PAIRS, each_pair, 0)

    def project_back(step):
        def body(start, size):
            rows = at_rows(start, size)
            hat, rho = normalize(state[step, rows, :])
            normed_low = (hat * vector(0) + vector(1)).astype(bf16)
            normed_grad = jnp.zeros((size, D), f32)
            for j in range(3):
                grads = projected_grad[rows, D * j : D * (j + 1)]
                qkv_sum[j] += dot_tn(normed_low, grads)
                normed_grad = normed_grad + dot_nt(grads, weight_qkv(j))
            add_vector(0, column_sum(normed_grad * hat))
            add_vector(1, column_sum(normed_grad))
            through = norm_backward(normed_grad, hat, rho, vector(0))
            direct = jnp.where(step == 1, state[2, rows, :], 0.0)
            carry[rows, :] = jnp.where(row_index(start, size) < length, carry[rows, :] + through + direct, 0.0)

        over_rows(length, SIZES_LENGTH, body)

    def backward(back_step, carried):
        step = 1 - back_step

        @pl.when(step == 0)
        def _():
            fetch().wait()

        feed_back(step)

        @pl.when(step == 1)
        def _():
            fetch().start()

        attend_back(step)
        project_back(step)
        return carried

    lax.fori_loop(0, 2, backward, 0)

    def place(row, rows, value):
        while rows:
            chunk, inside = divmod(row, CHUNK)
            some = min(rows, CHUNK - inside)
            at = PACKED * chunk + inside
            hidden[at : at + some, :] = value[:some]
            value, row, rows = value[some:], row + some, rows - some

    for j in range(3):
        for n in range(8):
            place(CHUNK * n + 64 * j, 64, qkv_sum[j, 64 * n : 64 * (n + 1), :].astype(bf16))
    place(1536, 512, out_sum[...].astype(bf16))
    for j in range(4):
        for at, rows, first in UP_SEGMENTS:
            place(2048 + at + rows * j, rows, up_sum[j, first : first + rows, :].astype(bf16))

    def place_down(j, carried):
        value = down_sum[j].T.astype(bf16)
        for part in range(D // 64):
            row = 4096 + D * j + 64 * part
            at = pl.multiple_of(row // CHUNK * PACKED + row % CHUNK, 16)
            hidden[pl.ds(at, 64), :] = value[64 * part : 64 * (part + 1)]
        return carried

    lax.fori_loop(0, 4, place_down, 0)
    for n in range(DEVICES):
        extra = next_rows(n, qkv_sum, out_sum, up_sum, hidden, vector_sum).astype(bf16)
        hidden[PACKED * n + CHUNK : PACKED * (n + 1), :] = extra
    copies = []
    for dc in range(2):
        part_a, part_b = (keep_a, keep_b) if dc == 0 else (send_a, send_b)
        for plane, (dy, dx) in enumerate(PLANE):
            for dz in range(4):
                row = pl.multiple_of(chunk_of(meta, dy, dc, dz, dx) * PACKED, 16)
                for part, index, first, some in (
                    (part_a, 4 * dz + plane, 0, ROWS_A),
                    (part_b, 4 * plane + dz, ROWS_A, ROWS_B),
                ):
                    copy = pltpu.make_async_copy(
                        hidden.at[pl.ds(row + first, some), :], part.at[index], out_sem.at[len(copies)]
                    )
                    copy.start()
                    copies.append(copy)
    for copy in copies:
        copy.wait()


def layer(meta, states, cotangent, pieces):
    in_place = pl.BlockSpec(memory_space=pltpu.VMEM)
    outside = pl.BlockSpec(memory_space=pl.ANY)
    outputs = pl.pallas_call(
        layer_kernel,
        out_shape=(
            shape_of(SEQ, D),
            shape_of(SEQ, D),
            shape_of(16, ROWS_A, D, dtype=bf16),
            shape_of(16, ROWS_A, D, dtype=bf16),
            shape_of(16, ROWS_B, D, dtype=bf16),
            shape_of(16, ROWS_B, D, dtype=bf16),
            shape_of(8 * SEQ, D, dtype=bf16),
        ),
        in_specs=[pl.BlockSpec(memory_space=pltpu.SMEM)] + [in_place] * 2 + [outside] * 16,
        out_specs=(in_place, in_place) + (outside,) * 5,
        scratch_shapes=[
            pltpu.VMEM((DEVICES * CHUNK, D), bf16),
            pltpu.VMEM((DEVICES, EXTRA, D), bf16),
            pltpu.VMEM((EXTRA, D), f32),
            pltpu.VMEM((3, SEQ, D), f32),
            pltpu.VMEM((2, SEQ, 3 * D), bf16),
            pltpu.VMEM((2, SEQ, D), bf16),
            pltpu.VMEM((2, SEQ, D), f32),
            pltpu.VMEM((8 * SEQ, D), bf16),
            pltpu.VMEM((SEQ, D), bf16),
            pltpu.VMEM((SEQ, 3 * D), bf16),
            pltpu.VMEM((2, SEQ // UNIT, HEADS, UNIT), f32),
            pltpu.VMEM((SEQ // UNIT, HEADS, UNIT), f32),
            pltpu.VMEM((3, D, D), f32),
            pltpu.VMEM((D, D), f32),
            pltpu.VMEM((4, D, D), f32),
            pltpu.VMEM((4, D, D), f32),
            pltpu.VMEM((16, D), f32),
            pltpu.VMEM((8, D), f32),
            pltpu.VMEM((8, PAIR), f32),
            pltpu.VMEM((SEQ, PAIR), f32),
            pltpu.VMEM((SEQ, PAIR), f32),
            pltpu.VMEM((PAIR, SEQ), bf16),
            pltpu.SemaphoreType.DMA((96,)),
            pltpu.SemaphoreType.DMA,
            pltpu.SemaphoreType.DMA((64,)),
        ],
        compiler_params=pltpu.CompilerParams(vmem_limit_bytes=63 * 1024 * 1024),
        name="layer",
    )(meta, states, cotangent, *pieces)
    return outputs[0], outputs[1], outputs[2:6]


def to_chunks(flat):
    wide = flat[:QKV_END].reshape(8, 64, 3, D).transpose(0, 2, 1, 3).reshape(1536, D)
    up = flat[OUT_END:UP_END].reshape(512, 4, D)
    pieces = [up[first : first + rows].transpose(1, 0, 2).reshape(4 * rows, D) for _, rows, first in UP_SEGMENTS]
    return jnp.concatenate(
        [wide, flat[QKV_END:OUT_END].reshape(D, D), *pieces, flat[UP_END:DOWN_END].reshape(FF, D)], axis=0
    )


def from_chunks(rows):
    wide = rows[:1536].reshape(8, 3, 64, D).transpose(0, 2, 1, 3).reshape(-1)
    up = rows[2048:4096]
    pieces = [
        up[at : at + 4 * rows].reshape(4, rows, D).transpose(1, 0, 2).reshape(-1) for at, rows, _ in UP_SEGMENTS
    ]
    return jnp.concatenate([wide, rows[1536:2048].reshape(-1), *pieces, rows[4096:].reshape(-1)])


def row_tables():
    order = np.concatenate(
        [
            (np.arange(1536).reshape(8, 64, 3).transpose(0, 2, 1)).reshape(-1),
            np.arange(1536, 2048),
            *[
                2048 + 4 * first + np.arange(4 * rows).reshape(rows, 4).transpose(1, 0).reshape(-1)
                for _, rows, first in UP_SEGMENTS
            ],
            np.arange(4096, 6144),
        ]
    )
    source = np.full((DEVICES, CHUNK + EXTRA), -1, np.int32)
    target = np.tile(np.arange(CHUNK + EXTRA, dtype=np.int32), (DEVICES, 1))
    for n in range(DEVICES):
        source[n, :CHUNK] = order[CHUNK * n : CHUNK * (n + 1)] - CHUNK * n
        target[n, source[n, :CHUNK]] = np.arange(CHUNK)
        width = 3 if n + 1 < 8 else 4 if 11 <= n + 1 < 22 else 1
        for row in range(10):
            at = row if width == 1 else 4 * (row % width) + row // width
            source[n, CHUNK + at] = CHUNK + row
    return source, target


def pick_rows(table, device, rows, precision=None):
    wanted = lax.dynamic_slice(jnp.asarray(table), (device, 0), (1, CHUNK + EXTRA)).reshape(-1, 1)
    pick = (wanted == iota((CHUNK + EXTRA, CHUNK + EXTRA), 1)).astype(rows.dtype)
    return jnp.dot(pick, rows, precision=precision, preferred_element_type=f32)


def send(array, dy=0, dx=0, dz=0, dc=0):
    pairs = []
    for y in range(2):
        for c in range(2):
            for z in range(4):
                for x in range(2):
                    other = (((y ^ dy) * 2 + (c ^ dc)) * 4 + (z ^ dz)) * 2 + (x ^ dx)
                    pairs.append((((y * 2 + c) * 4 + z) * 2 + x, other))
    return lax.ppermute(array, ("dp", "fsdp"), pairs)


def gather_weights(params, device, meanwhile):
    source, _ = row_tables()
    shift = (NPARAM // DEVICES - CHUNK * D) * device
    edge = jnp.zeros((EXTRA * D,), bf16)
    line = jnp.concatenate([edge, params.astype(bf16), edge])
    rows = lax.dynamic_slice(line, (EXTRA * D - shift,), ((CHUNK + EXTRA) * D,)).reshape(CHUNK + EXTRA, D)
    rows = pick_rows(source, device, rows).astype(bf16)
    own_a, own_b = rows[:ROWS_A], rows[ROWS_A:]
    first_a = jnp.stack([own_a] + [send(own_a, dy, dx) for dy, dx in PLANE[1:]])
    first_b = jnp.stack([own_b] + [send(own_b, dz=dz) for dz in (1, 2, 3)])
    first_a, first_b, meanwhile = lax.optimization_barrier((first_a, first_b, meanwhile))
    all_b = [first_b] + [send(first_b, dy, dx) for dy, dx in PLANE[1:]]
    all_a = [first_a] + [send(first_a, dz=dz) for dz in (1, 2, 3)]
    other_a = [send(part, dc=1) for part in all_a]
    other_b = [send(part, dc=1) for part in all_b]
    return all_a + other_a + all_b + other_b, meanwhile


def cut_weights(flat):
    chunks = to_chunks(flat[:DOWN_END]).reshape(DEVICES, CHUNK, D)
    extra = jnp.zeros((DEVICES, EXTRA, D), bf16).at[DEVICES - 1, :10].set(flat[DOWN_END:].reshape(10, D))
    chunks = jnp.concatenate([chunks, extra], axis=1).reshape(2, 2, 4, 2, PACKED, D)
    parts_a = chunks[..., :ROWS_A, :].transpose(1, 2, 3, 0, 4, 5).reshape(8, 4, ROWS_A, D)
    parts_b = chunks[..., ROWS_A:, :].transpose(1, 3, 0, 2, 4, 5).reshape(8, 4, ROWS_B, D)
    return [parts_a[n] for n in range(8)] + [parts_b[n] for n in range(8)]


def reduce_grads(parts, device, place, final_states, input_grad):
    keep_a, send_a, keep_b, send_b = parts
    _, target = row_tables()
    core_b, core_a = send(send_b, dc=1), send(send_a, dc=1)
    final_states = restore(place, final_states, "restore_final")
    core_a, final_states = lax.optimization_barrier((core_a, final_states))
    pair_a = [keep_a[4 * n : 4 * n + 4] + core_a[4 * n : 4 * n + 4] for n in range(4)]
    pair_b = [keep_b[4 * n : 4 * n + 4] + core_b[4 * n : 4 * n + 4] for n in range(4)]
    got_a = [send(pair_a[dz], dz=dz) for dz in (1, 2, 3)]
    got_b = [send(pair_b[n], *PLANE[n]) for n in (1, 2, 3)]
    line_a = sum((part.astype(f32) for part in got_a), pair_a[0].astype(f32))
    plane_b = sum((part.astype(f32) for part in got_b), pair_b[0].astype(f32))
    line_a, plane_b, input_grad = lax.optimization_barrier((line_a, plane_b, input_grad))
    got_b = [send(plane_b[dz].astype(bf16), dz=dz) for dz in (1, 2, 3)]
    got_a = [send(line_a[n].astype(bf16), *PLANE[n]) for n in (1, 2, 3)]
    input_grad = restore(place, input_grad, "restore_grad")
    got_a, got_b, input_grad = lax.optimization_barrier((got_a, got_b, input_grad))
    own_a = sum((part.astype(f32) for part in got_a), line_a[0])
    own_b = sum((part.astype(f32) for part in got_b), plane_b[0])
    rows = pick_rows(target, device, jnp.concatenate([own_a, own_b], axis=0), lax.Precision.HIGHEST)
    shift = (NPARAM // DEVICES - CHUNK * D) * device
    return lax.dynamic_slice(rows.reshape(-1), (shift,), (NPARAM // DEVICES,)), final_states, input_grad


def sum_all(value):
    value = jnp.broadcast_to(value, (8, 128))
    value = value + send(value, dc=1)
    value = value + sum(send(value, dy, dx) for dy, dx in PLANE[1:])
    return (value + sum(send(value, dz=dz) for dz in (1, 2, 3)))[0, 0]


def flat_grads(parts):
    keep_a, send_a, keep_b, send_b = parts
    chunks_a = jnp.stack([keep_a, send_a]).reshape(2, 4, 2, 2, ROWS_A, D).transpose(3, 0, 1, 2, 4, 5)
    chunks_b = jnp.stack([keep_b, send_b]).reshape(2, 2, 2, 4, ROWS_B, D).transpose(2, 0, 3, 1, 4, 5)
    chunks = jnp.concatenate(
        [chunks_a.reshape(DEVICES, ROWS_A, D), chunks_b.reshape(DEVICES, ROWS_B, D)], axis=1
    )
    rows = chunks[:, :CHUNK].reshape(DEVICES * CHUNK, D)
    vectors = chunks[DEVICES - 1, CHUNK : CHUNK + 10].reshape(-1)
    return jnp.concatenate([from_chunks(rows), vectors]).astype(f32)


def local(ways, states, params, first_moment, second_moment, ema_params, lengths, halt_counts, cotangent):
    both = ("dp", "fsdp")
    device = lax.axis_index(both)
    blockwise = ways == (4, 8)
    if blockwise:
        outer, inner = lax.axis_index("dp"), lax.axis_index("fsdp")
        place_index = jnp.stack([outer // 2, outer % 2, inner // 2, inner % 2]).astype(i32)
    else:
        place_index = jnp.zeros((4,), i32)
    prepared = prepare(lengths, place_index, halt_counts, states[0], cotangent[0])
    if blockwise:
        pieces, prepared = gather_weights(params, device, prepared)
    else:
        pieces = cut_weights(lax.all_gather(params.astype(bf16), both, axis=0, tiled=True))
    place, sorted_states, sorted_cotangent, meta = prepared
    final_states, input_grad, parts = layer(meta, sorted_states, sorted_cotangent, pieces)
    if blockwise:
        reduced, final_states, input_grad = reduce_grads(parts, device, place, final_states, input_grad)
        square_sum = sum_all(jnp.sum(reduced * reduced))
    else:
        final_states = restore(place, final_states, "restore_final")
        input_grad = restore(place, input_grad, "restore_grad")
        reduced = lax.psum_scatter(flat_grads(parts), both, scatter_dimension=0, tiled=True)
        square_sum = lax.psum(jnp.sum(reduced * reduced), both)
    grad_norm = jnp.sqrt(square_sum)
    clip_bound = NPARAM**0.5
    clipped = reduced * (clip_bound / jnp.maximum(grad_norm, clip_bound))
    new_first = BETA_FIRST * first_moment + (1.0 - BETA_FIRST) * clipped
    new_second = BETA_SECOND * second_moment + (1.0 - BETA_SECOND) * clipped * clipped
    first_hat = new_first / (1.0 - BETA_FIRST**ADAM_STEP)
    second_hat = new_second / (1.0 - BETA_SECOND**ADAM_STEP)
    shard_length = params.shape[0]
    index_all = device * shard_length + iota((shard_length,), 0)
    matrix = index_all < DOWN_END
    step_rate = jnp.where(matrix, RATE_MATRIX, RATE_VECTOR)
    decay_rate = jnp.where(matrix, WEIGHT_DECAY, 0.0)
    new_params = params - step_rate * (first_hat / (jnp.sqrt(second_hat) + ADAM_EPSILON) + decay_rate * params)
    average_decay = min(EMA_DECAY, (1.0 + ADAM_STEP) / (10.0 + ADAM_STEP))
    new_ema = average_decay * ema_params + (1.0 - average_decay) * new_params
    return (
        final_states[None],
        input_grad[None],
        clipped,
        grad_norm.reshape(1),
        new_params,
        new_first,
        new_second,
        new_ema,
        new_params.astype(bf16),
    )


def solution(mesh):
    both = ("dp", "fsdp")
    wide, flat, counts = P(both, None, None), P(both), P(both, None)
    ways = (mesh.shape["dp"], mesh.shape["fsdp"])
    return jax.shard_map(
        functools.partial(local, ways),
        mesh=mesh,
        in_specs=(wide, flat, flat, flat, flat, flat, counts, wide),
        out_specs=(wide, wide, flat, P(), flat, flat, flat, flat, flat),
        check_vma=False,
    )
```

```python
import functools
import math

import jax
import jax.numpy as jnp
import numpy as np
from jax import lax
from jax.experimental import pallas as pl
from jax.experimental.pallas import tpu as pltpu
from jax.sharding import PartitionSpec as P

D = 512
FF = 2048
HEADS = 8
SEQ = 1024
ADAM_STEP = 4
QKV_END = 786432
OUT_END = 1048576
UP_END = 2097152
DOWN_END = 3145728
NPARAM = 3150848

NORM_EPSILON = 1e-05
HALT_SHIFT = -1.0
BETA_FIRST = 0.9
BETA_SECOND = 0.999
ADAM_EPSILON = 1e-08
EMA_DECAY = 0.999
WEIGHT_DECAY = 0.1
RATE_MATRIX = 0.1
RATE_VECTOR = 1.0

BLOCK = 256
BLOCKS = SEQ // BLOCK
UNIT = 128
SIZES_LENGTH = (512,)
SIZES_ATTEND = (256, 128)
SIZES_SHIFTED = (128,)
SIZES_ATTEND_BACK = (256,)
SIZES_FEED = (512, 128)
SIZES_BACK = (512, 128)
PAIRS = HEADS // 2
PAIR = 128
SCORE_SCALE = 0.125
SCORE_LOG2 = SCORE_SCALE * math.log2(math.e)

f32 = jnp.float32
bf16 = jnp.bfloat16
i32 = jnp.int32

CHUNK = 192
DEVICES = 32
ROWS_A = 64
ROWS_B = 144
EXTRA = 16
PACKED = CHUNK + EXTRA
PLANE = [(0, 0), (1, 0), (0, 1), (1, 1)]
UP_SEGMENTS = [(0, 16, 0)] + [(64 + CHUNK * n, 48, 16 + 48 * n) for n in range(10)] + [(64 + CHUNK * 10, 16, 496)]


def dot(left, right):
    return jnp.dot(left, right, preferred_element_type=f32)


def dot_nt(left, right):
    return lax.dot_general(left, right, (((1,), (1,)), ((), ())), preferred_element_type=f32)


def dot_tn(left, right):
    return lax.dot_general(left, right, (((0,), (0,)), ((), ())), preferred_element_type=f32)


def iota(shape, axis):
    return lax.broadcasted_iota(i32, shape, axis)


def normalize(inputs):
    centred = inputs - jnp.mean(inputs, axis=-1, keepdims=True)
    rho = lax.rsqrt(jnp.mean(centred * centred, axis=-1, keepdims=True) + NORM_EPSILON)
    return centred * rho, rho


def norm_backward(grad_out, hat, rho, gain):
    grad_hat = grad_out * gain
    return rho * (
        grad_hat
        - jnp.mean(grad_hat, axis=-1, keepdims=True)
        - hat * jnp.mean(grad_hat * hat, axis=-1, keepdims=True)
    )


def gelu_parts(pre):
    cumulative = 0.5 + 0.5 * lax.erf(pre * 0.7071067811865476)
    density = jnp.exp2(pre * pre * (-0.5 * math.log2(math.e))) * 0.3989422804014327
    return pre * cumulative, cumulative + pre * density


def qkv_weight(ref, j):
    return jnp.concatenate([ref[CHUNK * n + 64 * j : CHUNK * n + 64 * (j + 1), :] for n in range(8)], axis=0)


def up_weight(ref, j):
    return jnp.concatenate(
        [ref[2048 + at + rows * j : 2048 + at + rows * (j + 1), :] for at, rows, _ in UP_SEGMENTS], axis=0
    )


def prepare_kernel(
    length_ref, index_ref, count_ref, state_ref, cotangent_ref, place_ref, states_out, cotangent_out, meta_ref
):
    length = length_ref[0]
    token = iota((1, SEQ), 1)
    valid = token < length
    two = jnp.where(valid & (count_ref[...] >= 2), 1.0, 0.0)
    one = jnp.where(valid & (count_ref[...] < 2), 1.0, 0.0)
    masks = jnp.concatenate([two, one, jnp.zeros((6, SEQ), f32)], axis=0).astype(bf16)
    earlier = jnp.where(iota((SEQ, SEQ), 0) < iota((SEQ, SEQ), 1), 1.0, 0.0).astype(bf16)
    ranks = dot(masks, earlier)
    n_two = jnp.sum(two)
    place = jnp.where(
        two > 0.0, ranks[0:1, :], jnp.where(one > 0.0, n_two + ranks[1:2, :], token.astype(f32))
    )
    place_ref[...] = jnp.broadcast_to(place, (8, SEQ))
    meta_ref[0] = n_two.astype(i32)
    meta_ref[1] = length
    for n in range(4):
        meta_ref[2 + n] = index_ref[n]

    def sort(block, carried):
        rows = pl.ds(pl.multiple_of(block * BLOCK, BLOCK), BLOCK)
        pick = jnp.where((iota((BLOCK, SEQ), 0) + block * BLOCK).astype(f32) == place, 1.0, 0.0).astype(bf16)
        states_out[rows, :] = dot(pick, state_ref[...]).astype(bf16)
        cotangent_out[rows, :] = dot(pick, cotangent_ref[...]).astype(bf16)
        return carried

    lax.fori_loop(0, BLOCKS, sort, 0)


def prepare(lengths, place_index, counts, states, cotangent):
    return pl.pallas_call(
        prepare_kernel,
        out_shape=(
            jax.ShapeDtypeStruct((8, SEQ), f32),
            jax.ShapeDtypeStruct((SEQ, D), bf16),
            jax.ShapeDtypeStruct((SEQ, D), bf16),
            jax.ShapeDtypeStruct((6,), i32),
        ),
        in_specs=[
            pl.BlockSpec(memory_space=pltpu.SMEM),
            pl.BlockSpec(memory_space=pltpu.SMEM),
            pl.BlockSpec(memory_space=pltpu.VMEM),
            pl.BlockSpec(memory_space=pltpu.VMEM),
            pl.BlockSpec(memory_space=pltpu.VMEM),
        ],
        out_specs=(
            pl.BlockSpec(memory_space=pltpu.VMEM),
            pl.BlockSpec(memory_space=pltpu.VMEM),
            pl.BlockSpec(memory_space=pltpu.VMEM),
            pl.BlockSpec(memory_space=pltpu.SMEM),
        ),
        cost_estimate=pl.CostEstimate(flops=6 * 10**9, transcendentals=0, bytes_accessed=4 * 10**6),
        name="prepare",
    )(lengths, place_index, counts, states, cotangent)


def restore_kernel(place_ref, sorted_ref, out_ref, columns, high, lower):
    columns[...] = jnp.broadcast_to(place_ref[0:1, :], (PAIR, SEQ)).T
    high[...] = sorted_ref[...].astype(bf16)
    lower[...] = (sorted_ref[...] - high[...].astype(f32)).astype(bf16)

    def unsort(block, carried):
        rows = pl.ds(pl.multiple_of(block * BLOCK, BLOCK), BLOCK)
        pick = jnp.concatenate(
            [
                jnp.where(columns[rows, :] == (iota((BLOCK, PAIR), 1) + PAIR * n).astype(f32), 1.0, 0.0).astype(bf16)
                for n in range(SEQ // PAIR)
            ],
            axis=1,
        )
        out_ref[rows, :] = dot(pick, high[...]) + dot(pick, lower[...])
        return carried

    lax.fori_loop(0, BLOCKS, unsort, 0)


def restore(place, array, name):
    return pl.pallas_call(
        restore_kernel,
        out_shape=jax.ShapeDtypeStruct((SEQ, D), f32),
        in_specs=[pl.BlockSpec(memory_space=pltpu.VMEM)] * 2,
        out_specs=pl.BlockSpec(memory_space=pltpu.VMEM),
        scratch_shapes=[pltpu.VMEM((SEQ, PAIR), f32), pltpu.VMEM((SEQ, D), bf16), pltpu.VMEM((SEQ, D), bf16)],
        cost_estimate=pl.CostEstimate(flops=6 * 10**9, transcendentals=0, bytes_accessed=4 * 10**6),
        name=name,
    )(place, array)


def next_rows(chunk, qkv_sum, out_sum, up_sum, packed, vector_sum):
    after = chunk + 1
    if after == DEVICES:
        return vector_sum[...]
    if after < 8:
        blocks = [qkv_sum[j, 64 * after : 64 * after + 8, :] for j in range(3)]
    elif after < 11:
        at = CHUNK * after - 1536
        return out_sum[at : at + 16, :]
    elif after < 22:
        first = 16 + 48 * (after - 11)
        blocks = [up_sum[j, first : first + 8, :] for j in range(4)]
    else:
        return packed[PACKED * after : PACKED * after + 16, :].astype(f32)
    width = len(blocks)
    rows = [blocks[r % width][r // width : r // width + 1, :] for r in range(10)]
    return jnp.concatenate(rows + [jnp.zeros((6, D), f32)], axis=0)


def chunk_of(meta, dy, dc, dz, dx):
    return (((meta[2] ^ dy) * 2 + (meta[3] ^ dc)) * 4 + (meta[4] ^ dz)) * 2 + (meta[5] ^ dx)


def shape_of(*shape, dtype=f32):
    return jax.ShapeDtypeStruct(shape, dtype)


def column_sum(array):
    return jnp.sum(array, axis=0, keepdims=True)


def layer_kernel(meta, states_ref, cotangent_ref, *refs):
    pieces = refs[:16]
    (
        final_out, carry, keep_a, send_a, keep_b, send_b, spill,
        matrices, extras, vectors,
        state, projected, mixed, middle, hidden, mixed_grad, projected_grad, logs, centres,
        qkv_sum, out_sum, up_sum, down_sum, vector_sum, first_key, norm_peak, key_sum, value_sum, turned, in_sem, spill_sem, out_sem,
    ) = refs[16:]
    n_two, length = meta[0], meta[1]
    lower = iota((1, PAIR), 1) < 64
    own = [lower, ~lower]

    def at_rows(start, size):
        return pl.ds(pl.multiple_of(start, UNIT), size)

    def hidden_rows(j, start, size):
        return pl.ds(pl.multiple_of(j * SEQ + start, UNIT), size)

    def over_rows(rows, sizes, body):
        def loop(first, size, count):
            def step(n, carried):
                body(first + n * size, size)
                return carried

            lax.fori_loop(0, count, step, 0)
            return first + count * size

        large = sizes[0]
        if len(sizes) == 1:
            return loop(0, large, (rows + large - 1) // large)
        covered = loop(0, large, (rows + large // 2 - 1) // large)
        return loop(covered, sizes[1], (jnp.maximum(rows - covered, 0) + sizes[1] - 1) // sizes[1])

    def rest_rows(covered, body):
        def step(n, carried):
            body(n * UNIT, UNIT)
            return carried

        lax.fori_loop(covered // UNIT, SEQ // UNIT, step, 0)

    def weight_qkv(j):
        return qkv_weight(matrices, j)

    def weight_out():
        return matrices[1536:2048, :]

    def weight_up(j):
        return up_weight(matrices, j)

    def weight_down(j):
        return matrices[4096 + D * j : 4096 + D * (j + 1), :]

    def vector(index):
        return vectors[index : index + 1, :]

    def add_vector(index, value):
        vector_sum[index : index + 1, :] += value

    def query_rows(step):
        return jnp.where(step == 0, length, n_two)

    def row_index(start, size):
        return iota((size, 1), 0) + start

    arriving = []
    for dc in range(2):
        for plane, (dy, dx) in enumerate(PLANE):
            for dz in range(4):
                chunk = chunk_of(meta, dy, dc, dz, dx)
                row = pl.multiple_of(chunk * CHUNK, CHUNK)
                part_a, part_b = pieces[4 * dc + dz].at[plane], pieces[8 + 4 * dc + plane].at[dz]
                for source, target in (
                    (part_a, matrices.at[pl.ds(row, ROWS_A), :]),
                    (part_b.at[: CHUNK - ROWS_A, :], matrices.at[pl.ds(row + ROWS_A, CHUNK - ROWS_A), :]),
                    (part_b.at[CHUNK - ROWS_A :, :], extras.at[chunk]),
                ):
                    copy = pltpu.make_async_copy(source, target, in_sem.at[len(arriving)])
                    copy.start()
                    arriving.append(copy)

    def start_rows(n, carried):
        rows = at_rows(n * UNIT, UNIT)
        state[0, rows, :] = states_ref[rows, :].astype(f32)
        state[1, rows, :] = jnp.zeros((UNIT, D), f32)
        mixed[0, rows, :] = jnp.zeros((UNIT, D), bf16)
        mixed[1, rows, :] = jnp.zeros((UNIT, D), bf16)
        mixed_grad[rows, :] = jnp.zeros((UNIT, D), bf16)
        return carried

    lax.fori_loop(0, SEQ // UNIT, start_rows, 0)

    def start_sums(n, carried):
        rows = at_rows(n * UNIT, UNIT)
        for total in (qkv_sum, up_sum, down_sum):
            for j in range(total.shape[0]):
                total[j, rows, :] = jnp.zeros((UNIT, D), f32)
        out_sum[rows, :] = jnp.zeros((UNIT, D), f32)
        return carried

    lax.fori_loop(0, D // UNIT, start_sums, 0)
    vector_sum[...] = jnp.zeros_like(vector_sum)
    centres[...] = jnp.zeros_like(centres)
    logs[...] = jnp.full_like(logs, 1e30)
    for copy in arriving:
        copy.wait()

    def complete(row, value):
        rows = value.shape[0]
        matrices[row : row + rows, :] = (matrices[row : row + rows, :].astype(f32) + value).astype(bf16)

    for n in range(1, DEVICES):
        value = extras[n - 1].astype(f32)
        if n < 8 or 11 <= n < 22:
            width, stride = (3, 64) if n < 8 else (4, 48 if n < 21 else 16)
            for j in range(width):
                rows = jnp.concatenate([value[4 * j : 4 * j + 4, :], jnp.zeros((4, D), f32)], axis=0)
                complete(CHUNK * n + stride * j, rows)
        else:
            complete(CHUNK * n, value)
    vectors[...] = extras[DEVICES - 1].astype(f32)

    heads = jnp.where(iota((D, PAIR), 0) // 64 == iota((D, PAIR), 1), 1.0, 0.0).astype(bf16)

    def project(step):
        def body(start, size):
            rows = at_rows(start, size)
            hat, _ = normalize(state[step, rows, :])
            normed_low = (hat * vector(0) + vector(1)).astype(bf16)
            queries = dot(normed_low, weight_qkv(0))
            projected[step, rows, 0:D] = queries.astype(bf16)
            keys = dot(normed_low, weight_qkv(1))
            for index, array in enumerate((queries, keys)):
                norms = dot((array * array).astype(bf16), heads)
                norm_peak[index : index + 1, :] = jnp.maximum(
                    norm_peak[index : index + 1, :], jnp.max(norms, axis=0, keepdims=True)
                )

            @pl.when(start == 0)
            def _():
                first_key[...] = jnp.broadcast_to(keys[0:1, :], first_key.shape)

            inside = row_index(start, size) < length
            projected[step, rows, D : 2 * D] = jnp.where(inside, keys, first_key[0:1, :]).astype(bf16)
            values = dot(normed_low, weight_qkv(2))
            projected[step, rows, 2 * D : 3 * D] = jnp.where(inside, values, 0.0).astype(bf16)

        def fill(start, size):
            rows = at_rows(start, size)
            projected[step, rows, D : 2 * D] = jnp.broadcast_to(first_key[0:1, :], (size, D)).astype(bf16)
            projected[step, rows, 2 * D : 3 * D] = jnp.zeros((size, D), bf16)

        norm_peak[...] = jnp.zeros_like(norm_peak)
        rest_rows(over_rows(length, SIZES_LENGTH, body), fill)

    def attend_pair(step, start, size, pair, shifted):
        rows = at_rows(start, size)
        ones = jnp.where(iota((SEQ, 1), 0) < length, 1.0, 0.0).astype(bf16)
        def lanes(offset):
            at = offset + pair * PAIR
            return pl.ds(at if isinstance(at, int) else pl.multiple_of(at, PAIR), PAIR)

        queries = projected[step, rows, lanes(0)]
        keys = projected[step, :, lanes(D)]
        values = projected[step, :, lanes(2 * D)]
        peaks, sums = [], []
        for half in range(2):
            scores = dot_nt(jnp.where(own[half], queries, jnp.zeros_like(queries)), keys) * SCORE_LOG2
            if shifted:
                peaks.append(jnp.max(scores, axis=-1, keepdims=True))
                scores = scores - peaks[half]
            sums.append(dot(jnp.exp2(scores).astype(bf16), jnp.where(own[half], values, ones)))
        total = jnp.where(lower, pltpu.roll(sums[0], 64, 1), pltpu.roll(sums[1], 64, 1))
        mixed[step, rows, lanes(0)] = (jnp.where(lower, sums[0], sums[1]) / total).astype(bf16)
        log = jnp.log2(total)
        if shifted:
            log = log + jnp.where(lower, peaks[0], peaks[1])
        log = log.T
        for unit in range(size // UNIT):
            columns = slice(unit * UNIT, (unit + 1) * UNIT)
            logs[step, start // UNIT + unit, pl.ds(2 * pair, 1), :] = log[0:1, columns]
            logs[step, start // UNIT + unit, pl.ds(2 * pair + 1, 1), :] = log[64:65, columns]

    def attend(step):
        bound = jnp.max(norm_peak[0:1, :] * norm_peak[1:2, :])
        plain = bound * (1.02 * SCORE_LOG2) ** 2 < 60.0**2

        @pl.when(plain)
        def _():
            def body(start, size):
                def each(pair, carried):
                    attend_pair(step, start, size, pair, False)
                    return carried

                if size == SIZES_ATTEND[0]:
                    for pair in range(PAIRS):
                        each(pair, 0)
                else:
                    lax.fori_loop(0, PAIRS, each, 0)

            over_rows(query_rows(step), SIZES_ATTEND, body)

        @pl.when(~plain)
        def _():
            def body(start, size):
                def each(pair, carried):
                    attend_pair(step, start, size, pair, True)
                    return carried

                lax.fori_loop(0, PAIRS, each, 0)

            over_rows(query_rows(step), SIZES_SHIFTED, body)

    def feed_forward(step):
        def body(start, size):
            rows = at_rows(start, size)
            between = state[step, rows, :] + dot(mixed[step, rows, :], weight_out())
            middle[step, rows, :] = between
            hat, _ = normalize(between)
            normed_low = (hat * vector(2) + vector(3)).astype(bf16)
            output = between + vector(4)
            for j in range(4):
                value, slope = gelu_parts(dot(normed_low, weight_up(j)) + vector(6 + j))
                value_low = value.astype(bf16)
                hidden[hidden_rows(j, start, size), :] = value_low
                hidden[hidden_rows(4 + j, start, size), :] = slope.astype(bf16)
                output = output + dot(value_low, weight_down(j))
            state[step + 1, rows, :] = output

        over_rows(query_rows(step), SIZES_FEED, body)

    def save():
        return pltpu.make_async_copy(hidden, spill, spill_sem)

    def fetch():
        return pltpu.make_async_copy(spill, hidden, spill_sem)

    def forward(step, carried):
        project(step)
        attend(step)

        @pl.when(step == 1)
        def _():
            save().wait()

        feed_forward(step)

        @pl.when(step == 0)
        def _():
            save().start()

        return carried

    lax.fori_loop(0, 2, forward, 0)

    def mix(start, size):
        rows = at_rows(start, size)
        row = row_index(start, size)
        two, valid = row < n_two, row < length
        before = state[1, rows, :]
        after = jnp.where(two, state[2, rows, :], before)
        halting = jax.nn.sigmoid(jnp.sum(before * vector(5), axis=-1, keepdims=True) + HALT_SHIFT)
        share_one = jnp.where(two, halting, 1.0)
        share_two = jnp.where(two, 1.0 - halting, 0.0)
        final_out[rows, :] = jnp.where(valid, share_one * before + share_two * after, 0.0)
        grad_final = jnp.where(valid, cotangent_ref[rows, :].astype(f32), 0.0)
        first_sum = jnp.sum(grad_final * before, axis=-1, keepdims=True)
        second_sum = jnp.sum(grad_final * after, axis=-1, keepdims=True)
        logit_grad = jnp.where(two, (first_sum - second_sum) * halting * (1.0 - halting), 0.0)
        add_vector(5, column_sum(jnp.where(valid, logit_grad * before, 0.0)))
        carry[rows, :] = share_two * grad_final
        state[2, rows, :] = jnp.where(valid, share_one * grad_final + logit_grad * vector(5), 0.0)

    def blank(start, size):
        rows = at_rows(start, size)
        final_out[rows, :] = jnp.zeros((size, D), f32)
        carry[rows, :] = jnp.zeros((size, D), f32)

    rest_rows(over_rows(length, SIZES_LENGTH, mix), blank)

    def feed_back(step):
        def body(start, size):
            rows = at_rows(start, size)
            grad = carry[rows, :]
            branch = grad.astype(bf16)
            add_vector(4, column_sum(branch.astype(f32)))
            hat, rho = normalize(middle[step, rows, :])
            normed_low = (hat * vector(2) + vector(3)).astype(bf16)
            normed_grad = jnp.zeros((size, D), f32)
            for j in range(4):
                slope = hidden[hidden_rows(4 + j, start, size), :].astype(f32)
                pre_grad = (dot_nt(branch, weight_down(j)) * slope).astype(bf16)
                add_vector(6 + j, column_sum(pre_grad.astype(f32)))
                down_sum[j] += dot_tn(branch, hidden[hidden_rows(j, start, size), :])
                normed_grad = normed_grad + dot_nt(pre_grad, weight_up(j))
                up_sum[j] += dot_tn(normed_low, pre_grad)
            add_vector(2, column_sum(normed_grad * hat))
            add_vector(3, column_sum(normed_grad))
            middle_grad = grad + norm_backward(normed_grad, hat, rho, vector(2))
            carry[rows, :] = middle_grad
            attended = middle_grad.astype(bf16)
            out_sum[...] += dot_tn(mixed[step, rows, :], attended)
            before_out = dot_nt(attended, weight_out()).astype(bf16)
            mixed_grad[rows, :] = before_out
            product = before_out.astype(f32) * mixed[step, rows, :].astype(f32)
            head = jnp.where(iota((HEADS, D), 1) // 64 == iota((HEADS, D), 0), 1.0, 0.0).astype(bf16)
            high = product.astype(bf16)
            centre = dot_nt(head, high) + dot_nt(head, (product - high.astype(f32)).astype(bf16))
            for unit in range(size // UNIT):
                centres[start // UNIT + unit] = centre[:, unit * UNIT : (unit + 1) * UNIT]

        over_rows(query_rows(step), SIZES_BACK, body)

    def attend_back(step):
        inside = iota((SEQ, 1), 0) < length

        def each_pair(pair, carried):
            def lanes(offset):
                return pl.ds(pl.multiple_of(offset + pair * PAIR, PAIR), PAIR)

            def clear(start, size):
                projected_grad[at_rows(start, size), lanes(0)] = jnp.zeros((size, PAIR), bf16)

            key_sum[...] = jnp.zeros_like(key_sum)
            value_sum[...] = jnp.zeros_like(value_sum)
            own_keys = projected[step, :, lanes(D)]
            turned[...] = jnp.where(inside, own_keys, jnp.zeros_like(own_keys)).T

            def body(start, size):
                rows = at_rows(start, size)
                keys, values = projected[step, :, lanes(D)], projected[step, :, lanes(2 * D)]
                queries, grads = projected[step, rows, lanes(0)], mixed_grad[rows, lanes(0)]
                query_half = [jnp.where(o, queries, jnp.zeros_like(queries)) for o in own]
                grad_half = [jnp.where(o, grads, jnp.zeros_like(grads)) for o in own]
                weights, slopes = [], []
                for h in range(2):
                    units = [start // UNIT + unit for unit in range(size // UNIT)]
                    log = jnp.concatenate([logs[step, unit, pl.ds(2 * pair + h, 1), :] for unit in units], axis=1)
                    centre = jnp.concatenate([centres[unit, pl.ds(2 * pair + h, 1), :] for unit in units], axis=1)
                    attention = jnp.exp2(dot_nt(keys, query_half[h]) * SCORE_LOG2 - log)
                    slope = (attention * (dot_nt(values, grad_half[h]) - centre)).astype(bf16)
                    weights.append(attention.astype(bf16))
                    slopes.append(slope)
                value_sum[...] += dot(jnp.concatenate(weights, axis=1), jnp.concatenate(grad_half, axis=0))
                key_sum[...] += dot(jnp.concatenate(slopes, axis=1), jnp.concatenate(query_half, axis=0))
                turned_grads = [dot(turned[64 * h : 64 * (h + 1), :], slopes[h]) for h in range(2)]
                projected_grad[rows, lanes(0)] = (jnp.concatenate(turned_grads, axis=0).T * SCORE_SCALE).astype(bf16)

            covered = over_rows(query_rows(step), SIZES_ATTEND_BACK, body)
            rest_rows(covered, clear)
            projected_grad[:, lanes(D)] = jnp.where(inside, key_sum[...] * SCORE_SCALE, 0.0).astype(bf16)
            projected_grad[:, lanes(2 * D)] = jnp.where(inside, value_sum[...], 0.0).astype(bf16)
            return carried

        lax.fori_loop(0, PAIRS, each_pair, 0)

    def project_back(step):
        def body(start, size):
            rows = at_rows(start, size)
            hat, rho = normalize(state[step, rows, :])
            normed_low = (hat * vector(0) + vector(1)).astype(bf16)
            normed_grad = jnp.zeros((size, D), f32)
            for j in range(3):
                grads = projected_grad[rows, D * j : D * (j + 1)]
                qkv_sum[j] += dot_tn(normed_low, grads)
                normed_grad = normed_grad + dot_nt(grads, weight_qkv(j))
            add_vector(0, column_sum(normed_grad * hat))
            add_vector(1, column_sum(normed_grad))
            through = norm_backward(normed_grad, hat, rho, vector(0))
            direct = jnp.where(step == 1, state[2, rows, :], 0.0)
            carry[rows, :] = jnp.where(row_index(start, size) < length, carry[rows, :] + through + direct, 0.0)

        over_rows(length, SIZES_LENGTH, body)

    def backward(back_step, carried):
        step = 1 - back_step

        @pl.when(step == 0)
        def _():
            fetch().wait()

        feed_back(step)

        @pl.when(step == 1)
        def _():
            fetch().start()

        attend_back(step)
        project_back(step)
        return carried

    lax.fori_loop(0, 2, backward, 0)

    def place(row, rows, value):
        while rows:
            chunk, inside = divmod(row, CHUNK)
            some = min(rows, CHUNK - inside)
            at = PACKED * chunk + inside
            hidden[at : at + some, :] = value[:some]
            value, row, rows = value[some:], row + some, rows - some

    for j in range(3):
        for n in range(8):
            place(CHUNK * n + 64 * j, 64, qkv_sum[j, 64 * n : 64 * (n + 1), :].astype(bf16))
    place(1536, 512, out_sum[...].astype(bf16))
    for j in range(4):
        for at, rows, first in UP_SEGMENTS:
            place(2048 + at + rows * j, rows, up_sum[j, first : first + rows, :].astype(bf16))

    def place_down(j, carried):
        value = down_sum[j].T.astype(bf16)
        for part in range(D // 64):
            row = 4096 + D * j + 64 * part
            at = pl.multiple_of(row // CHUNK * PACKED + row % CHUNK, 16)
            hidden[pl.ds(at, 64), :] = value[64 * part : 64 * (part + 1)]
        return carried

    lax.fori_loop(0, 4, place_down, 0)
    for n in range(DEVICES):
        extra = next_rows(n, qkv_sum, out_sum, up_sum, hidden, vector_sum).astype(bf16)
        hidden[PACKED * n + CHUNK : PACKED * (n + 1), :] = extra
    copies = []
    for dc in range(2):
        part_a, part_b = (keep_a, keep_b) if dc == 0 else (send_a, send_b)
        for plane, (dy, dx) in enumerate(PLANE):
            for dz in range(4):
                row = pl.multiple_of(chunk_of(meta, dy, dc, dz, dx) * PACKED, 16)
                for part, index, first, some in (
                    (part_a, 4 * dz + plane, 0, ROWS_A),
                    (part_b, 4 * plane + dz, ROWS_A, ROWS_B),
                ):
                    copy = pltpu.make_async_copy(
                        hidden.at[pl.ds(row + first, some), :], part.at[index], out_sem.at[len(copies)]
                    )
                    copy.start()
                    copies.append(copy)
    for copy in copies:
        copy.wait()


def layer(meta, states, cotangent, pieces):
    in_place = pl.BlockSpec(memory_space=pltpu.VMEM)
    outside = pl.BlockSpec(memory_space=pl.ANY)
    outputs = pl.pallas_call(
        layer_kernel,
        out_shape=(
            shape_of(SEQ, D),
            shape_of(SEQ, D),
            shape_of(16, ROWS_A, D, dtype=bf16),
            shape_of(16, ROWS_A, D, dtype=bf16),
            shape_of(16, ROWS_B, D, dtype=bf16),
            shape_of(16, ROWS_B, D, dtype=bf16),
            shape_of(8 * SEQ, D, dtype=bf16),
        ),
        in_specs=[pl.BlockSpec(memory_space=pltpu.SMEM)] + [in_place] * 2 + [outside] * 16,
        out_specs=(in_place, in_place) + (outside,) * 5,
        scratch_shapes=[
            pltpu.VMEM((DEVICES * CHUNK, D), bf16),
            pltpu.VMEM((DEVICES, EXTRA, D), bf16),
            pltpu.VMEM((EXTRA, D), f32),
            pltpu.VMEM((3, SEQ, D), f32),
            pltpu.VMEM((2, SEQ, 3 * D), bf16),
            pltpu.VMEM((2, SEQ, D), bf16),
            pltpu.VMEM((2, SEQ, D), f32),
            pltpu.VMEM((8 * SEQ, D), bf16),
            pltpu.VMEM((SEQ, D), bf16),
            pltpu.VMEM((SEQ, 3 * D), bf16),
            pltpu.VMEM((2, SEQ // UNIT, HEADS, UNIT), f32),
            pltpu.VMEM((SEQ // UNIT, HEADS, UNIT), f32),
            pltpu.VMEM((3, D, D), f32),
            pltpu.VMEM((D, D), f32),
            pltpu.VMEM((4, D, D), f32),
            pltpu.VMEM((4, D, D), f32),
            pltpu.VMEM((16, D), f32),
            pltpu.VMEM((8, D), f32),
            pltpu.VMEM((8, PAIR), f32),
            pltpu.VMEM((SEQ, PAIR), f32),
            pltpu.VMEM((SEQ, PAIR), f32),
            pltpu.VMEM((PAIR, SEQ), bf16),
            pltpu.SemaphoreType.DMA((96,)),
            pltpu.SemaphoreType.DMA,
            pltpu.SemaphoreType.DMA((64,)),
        ],
        compiler_params=pltpu.CompilerParams(vmem_limit_bytes=63 * 1024 * 1024),
        name="layer",
    )(meta, states, cotangent, *pieces)
    return outputs[0], outputs[1], outputs[2:6]


def to_chunks(flat):
    wide = flat[:QKV_END].reshape(8, 64, 3, D).transpose(0, 2, 1, 3).reshape(1536, D)
    up = flat[OUT_END:UP_END].reshape(512, 4, D)
    pieces = [up[first : first + rows].transpose(1, 0, 2).reshape(4 * rows, D) for _, rows, first in UP_SEGMENTS]
    return jnp.concatenate(
        [wide, flat[QKV_END:OUT_END].reshape(D, D), *pieces, flat[UP_END:DOWN_END].reshape(FF, D)], axis=0
    )


def from_chunks(rows):
    wide = rows[:1536].reshape(8, 3, 64, D).transpose(0, 2, 1, 3).reshape(-1)
    up = rows[2048:4096]
    pieces = [
        up[at : at + 4 * rows].reshape(4, rows, D).transpose(1, 0, 2).reshape(-1) for at, rows, _ in UP_SEGMENTS
    ]
    return jnp.concatenate([wide, rows[1536:2048].reshape(-1), *pieces, rows[4096:].reshape(-1)])


def row_tables():
    order = np.concatenate(
        [
            (np.arange(1536).reshape(8, 64, 3).transpose(0, 2, 1)).reshape(-1),
            np.arange(1536, 2048),
            *[
                2048 + 4 * first + np.arange(4 * rows).reshape(rows, 4).transpose(1, 0).reshape(-1)
                for _, rows, first in UP_SEGMENTS
            ],
            np.arange(4096, 6144),
        ]
    )
    source = np.full((DEVICES, CHUNK + EXTRA), -1, np.int32)
    target = np.tile(np.arange(CHUNK + EXTRA, dtype=np.int32), (DEVICES, 1))
    for n in range(DEVICES):
        source[n, :CHUNK] = order[CHUNK * n : CHUNK * (n + 1)] - CHUNK * n
        target[n, source[n, :CHUNK]] = np.arange(CHUNK)
        width = 3 if n + 1 < 8 else 4 if 11 <= n + 1 < 22 else 1
        for row in range(10):
            at = row if width == 1 else 4 * (row % width) + row // width
            source[n, CHUNK + at] = CHUNK + row
    return source, target


def pick_rows(table, device, rows, precision=None):
    wanted = lax.dynamic_slice(jnp.asarray(table), (device, 0), (1, CHUNK + EXTRA)).reshape(-1, 1)
    pick = (wanted == iota((CHUNK + EXTRA, CHUNK + EXTRA), 1)).astype(rows.dtype)
    return jnp.dot(pick, rows, precision=precision, preferred_element_type=f32)


def send(array, dy=0, dx=0, dz=0, dc=0):
    pairs = []
    for y in range(2):
        for c in range(2):
            for z in range(4):
                for x in range(2):
                    other = (((y ^ dy) * 2 + (c ^ dc)) * 4 + (z ^ dz)) * 2 + (x ^ dx)
                    pairs.append((((y * 2 + c) * 4 + z) * 2 + x, other))
    return lax.ppermute(array, ("dp", "fsdp"), pairs)


def gather_weights(params, device, meanwhile):
    source, _ = row_tables()
    shift = (NPARAM // DEVICES - CHUNK * D) * device
    line = lax.pad(params.astype(bf16), jnp.zeros((), bf16), [(EXTRA * D, EXTRA * D, 0)])
    rows = lax.dynamic_slice(line, (EXTRA * D - shift,), ((CHUNK + EXTRA) * D,)).reshape(CHUNK + EXTRA, D)
    rows = pick_rows(source, device, rows).astype(bf16)
    own_a, own_b = rows[:ROWS_A], rows[ROWS_A:]
    first_a = jnp.stack([own_a] + [send(own_a, dy, dx) for dy, dx in PLANE[1:]])
    first_b = jnp.stack([own_b] + [send(own_b, dz=dz) for dz in (1, 2, 3)])
    first_a, first_b, meanwhile = lax.optimization_barrier((first_a, first_b, meanwhile))
    all_b = [first_b] + [send(first_b, dy, dx) for dy, dx in PLANE[1:]]
    all_a = [first_a] + [send(first_a, dz=dz) for dz in (1, 2, 3)]
    other_a = [send(part, dc=1) for part in all_a]
    other_b = [send(part, dc=1) for part in all_b]
    return all_a + other_a + all_b + other_b, meanwhile


def cut_weights(flat):
    chunks = to_chunks(flat[:DOWN_END]).reshape(DEVICES, CHUNK, D)
    extra = jnp.zeros((DEVICES, EXTRA, D), bf16).at[DEVICES - 1, :10].set(flat[DOWN_END:].reshape(10, D))
    chunks = jnp.concatenate([chunks, extra], axis=1).reshape(2, 2, 4, 2, PACKED, D)
    parts_a = chunks[..., :ROWS_A, :].transpose(1, 2, 3, 0, 4, 5).reshape(8, 4, ROWS_A, D)
    parts_b = chunks[..., ROWS_A:, :].transpose(1, 3, 0, 2, 4, 5).reshape(8, 4, ROWS_B, D)
    return [parts_a[n] for n in range(8)] + [parts_b[n] for n in range(8)]


def finish_kernel(shift_ref, wanted_ref, own_a, a_one, a_two, a_three, own_b, b_one, b_two, b_three, rows_out, square_out):
    part_a = own_a[...] + a_one[...].astype(f32) + a_two[...].astype(f32) + a_three[...].astype(f32)
    part_b = own_b[...] + b_one[...].astype(f32) + b_two[...].astype(f32) + b_three[...].astype(f32)
    rows = jnp.concatenate([part_a, part_b], axis=0)
    pick = jnp.where(wanted_ref[...] == iota((PACKED, PACKED), 1), 1.0, 0.0).astype(bf16)
    high = rows.astype(bf16)
    rest = rows - high.astype(f32)
    middle = rest.astype(bf16)
    low = (rest - middle.astype(f32)).astype(bf16)
    rows = dot(pick, high) + dot(pick, middle) + dot(pick, low)
    rows_out[...] = rows
    index = iota((PACKED, D), 0) * D + iota((PACKED, D), 1) - shift_ref[0]
    own = (index >= 0) & (index < NPARAM // DEVICES)
    square_out[...] = jnp.full((8, 128), jnp.sum(jnp.where(own, rows * rows, 0.0)), f32)


def reduce_grads(parts, device, place, final_states, input_grad):
    keep_a, send_a, keep_b, send_b = parts
    _, target = row_tables()
    core_b, core_a = send(send_b, dc=1), send(send_a, dc=1)
    final_states = restore(place, final_states, "restore_final")
    core_a, final_states = lax.optimization_barrier((core_a, final_states))
    pair_a = [keep_a[4 * n : 4 * n + 4] + core_a[4 * n : 4 * n + 4] for n in range(4)]
    pair_b = [keep_b[4 * n : 4 * n + 4] + core_b[4 * n : 4 * n + 4] for n in range(4)]
    got_a = [send(pair_a[dz], dz=dz) for dz in (1, 2, 3)]
    got_b = [send(pair_b[n], *PLANE[n]) for n in (1, 2, 3)]
    line_a = sum((part.astype(f32) for part in got_a), pair_a[0].astype(f32))
    plane_b = sum((part.astype(f32) for part in got_b), pair_b[0].astype(f32))
    line_a, plane_b, input_grad = lax.optimization_barrier((line_a, plane_b, input_grad))
    got_b = [send(plane_b[dz].astype(bf16), dz=dz) for dz in (1, 2, 3)]
    got_a = [send(line_a[n].astype(bf16), *PLANE[n]) for n in (1, 2, 3)]
    input_grad = restore(place, input_grad, "restore_grad")
    got_a, got_b, input_grad = lax.optimization_barrier((got_a, got_b, input_grad))
    shift = (NPARAM // DEVICES - CHUNK * D) * device
    wanted = lax.dynamic_slice(jnp.asarray(target), (device, 0), (1, PACKED)).reshape(PACKED, 1)
    rows, square_sum = pl.pallas_call(
        finish_kernel,
        out_shape=(shape_of(PACKED, D), shape_of(8, 128)),
        in_specs=[pl.BlockSpec(memory_space=pltpu.SMEM)] + [pl.BlockSpec(memory_space=pltpu.VMEM)] * 9,
        out_specs=(pl.BlockSpec(memory_space=pltpu.VMEM),) * 2,
        name="finish",
    )(shift.astype(i32).reshape(1), wanted, line_a[0], *got_a, plane_b[0], *got_b)
    reduced = lax.dynamic_slice(rows.reshape(-1), (shift,), (NPARAM // DEVICES,))
    return reduced, sum_all(square_sum), final_states, input_grad


def sum_all(value):
    value = value + send(value, dc=1)
    value = value + sum(send(value, dy, dx) for dy, dx in PLANE[1:])
    return (value + sum(send(value, dz=dz) for dz in (1, 2, 3)))[0, 0]


def flat_grads(parts):
    keep_a, send_a, keep_b, send_b = parts
    chunks_a = jnp.stack([keep_a, send_a]).reshape(2, 4, 2, 2, ROWS_A, D).transpose(3, 0, 1, 2, 4, 5)
    chunks_b = jnp.stack([keep_b, send_b]).reshape(2, 2, 2, 4, ROWS_B, D).transpose(2, 0, 3, 1, 4, 5)
    chunks = jnp.concatenate(
        [chunks_a.reshape(DEVICES, ROWS_A, D), chunks_b.reshape(DEVICES, ROWS_B, D)], axis=1
    )
    rows = chunks[:, :CHUNK].reshape(DEVICES * CHUNK, D)
    vectors = chunks[DEVICES - 1, CHUNK : CHUNK + 10].reshape(-1)
    return jnp.concatenate([from_chunks(rows), vectors]).astype(f32)


def local(ways, states, params, first_moment, second_moment, ema_params, lengths, halt_counts, cotangent):
    both = ("dp", "fsdp")
    device = lax.axis_index(both)
    blockwise = ways == (4, 8)
    if blockwise:
        outer, inner = lax.axis_index("dp"), lax.axis_index("fsdp")
        place_index = jnp.stack([outer // 2, outer % 2, inner // 2, inner % 2]).astype(i32)
    else:
        place_index = jnp.zeros((4,), i32)
    prepared = prepare(lengths, place_index, halt_counts, states[0], cotangent[0])
    if blockwise:
        pieces, prepared = gather_weights(params, device, prepared)
    else:
        pieces = cut_weights(lax.all_gather(params.astype(bf16), both, axis=0, tiled=True))
    place, sorted_states, sorted_cotangent, meta = prepared
    final_states, input_grad, parts = layer(meta, sorted_states, sorted_cotangent, pieces)
    if blockwise:
        reduced, square_sum, final_states, input_grad = reduce_grads(parts, device, place, final_states, input_grad)
    else:
        final_states = restore(place, final_states, "restore_final")
        input_grad = restore(place, input_grad, "restore_grad")
        reduced = lax.psum_scatter(flat_grads(parts), both, scatter_dimension=0, tiled=True)
        square_sum = lax.psum(jnp.sum(reduced * reduced), both)
    grad_norm = jnp.sqrt(square_sum)
    clip_bound = NPARAM**0.5
    clipped = reduced * (clip_bound / jnp.maximum(grad_norm, clip_bound))
    new_first = BETA_FIRST * first_moment + (1.0 - BETA_FIRST) * clipped
    new_second = BETA_SECOND * second_moment + (1.0 - BETA_SECOND) * clipped * clipped
    first_hat = new_first / (1.0 - BETA_FIRST**ADAM_STEP)
    second_hat = new_second / (1.0 - BETA_SECOND**ADAM_STEP)
    shard_length = params.shape[0]
    index_all = device * shard_length + iota((shard_length,), 0)
    matrix = index_all < DOWN_END
    step_rate = jnp.where(matrix, RATE_MATRIX, RATE_VECTOR)
    decay_rate = jnp.where(matrix, WEIGHT_DECAY, 0.0)
    new_params = params - step_rate * (first_hat / (jnp.sqrt(second_hat) + ADAM_EPSILON) + decay_rate * params)
    average_decay = min(EMA_DECAY, (1.0 + ADAM_STEP) / (10.0 + ADAM_STEP))
    new_ema = average_decay * ema_params + (1.0 - average_decay) * new_params
    return (
        final_states[None],
        input_grad[None],
        clipped,
        grad_norm.reshape(1),
        new_params,
        new_first,
        new_second,
        new_ema,
        new_params.astype(bf16),
    )


def solution(mesh):
    both = ("dp", "fsdp")
    wide, flat, counts = P(both, None, None), P(both), P(both, None)
    ways = (mesh.shape["dp"], mesh.shape["fsdp"])
    return jax.shard_map(
        functools.partial(local, ways),
        mesh=mesh,
        in_specs=(wide, flat, flat, flat, flat, flat, counts, wide),
        out_specs=(wide, wide, flat, P(), flat, flat, flat, flat, flat),
        check_vma=False,
    )
```
